8 devices in a mesh: dp: 2 (over z, y), tp: 4 (over x, core).
Axes of the slice: x: 2, y: 2, z: 1, core: 2. Of those that a mesh axis runs over, the one named last changes fastest.
Arguments:
- x_stored: bfloat16 [6, 16, 1024, 1024], P(None, 'dp')
- u_stored: bfloat16 [6, 16, 1024, 4096], P(None, 'dp', None, 'tp')
- w_up: bfloat16 [6, 1024, 4096], P(None, None, 'tp')
- w_down: bfloat16 [6, 4096, 1024], P(None, 'tp')
- d_out: bfloat16 [16, 1024, 1024], P('dp')
- noise_up: float32 [6, 1024, 4096], P(None, 'dp', 'tp')
- noise_down: float32 [6, 4096, 1024], P(None, 'tp', 'dp')
- clip_up: float32 [6], replicated
- clip_down: float32 [6], replicated
- noise_mult: float32 [1], replicated
Outputs:
- output 1: float32 [6, 1024, 4096], P(None, 'dp', 'tp')
- output 2: float32 [6, 4096, 1024], P(None, 'tp', 'dp')
All inputs are finite; a program needn't handle non-finite values.
Results may differ from the reference program's by a relative error of at most 0.017855.
Values are sent between devices in bfloat16 or wider.
A program may use at most 1.25 GiB of HBM per device.

```python
import math
import jax
import jax.numpy as jnp
from jax import lax

NUM_LAYERS = 6
NUM_EXAMPLES = 16
SEQ_LEN = 1024
D_MODEL = 1024
D_FF = 4096

GELU_SCALE = math.sqrt(2.0 / math.pi)


def gelu_pair(pre_act):
    tanh_val = jnp.tanh(GELU_SCALE * (pre_act + 0.044715 * pre_act * pre_act * pre_act))
    gelu_val = 0.5 * pre_act * (1.0 + tanh_val)
    gelu_slope = 0.5 * (1.0 + tanh_val) + 0.5 * pre_act * (1.0 - tanh_val * tanh_val) * GELU_SCALE * (1.0 + 0.134145 * pre_act * pre_act)
    return gelu_val, gelu_slope


def setup_inputs(seed: int = 0) -> dict:
    key_list = jax.random.split(jax.random.key(seed), 11)
    x_stored = jax.random.normal(key_list[0], (NUM_LAYERS, NUM_EXAMPLES, SEQ_LEN, D_MODEL), jnp.float32).astype(jnp.bfloat16)
    u_stored = jax.random.normal(key_list[1], (NUM_LAYERS, NUM_EXAMPLES, SEQ_LEN, D_FF), jnp.float32).astype(jnp.bfloat16)
    w_up = (jax.random.normal(key_list[2], (NUM_LAYERS, D_MODEL, D_FF), jnp.float32) * D_MODEL ** -0.5).astype(jnp.bfloat16)
    w_down = (jax.random.normal(key_list[3], (NUM_LAYERS, D_FF, D_MODEL), jnp.float32) * D_FF ** -0.5).astype(jnp.bfloat16)
    row_scale = 2.0 ** jax.random.uniform(key_list[4], (NUM_EXAMPLES, 1, 1), jnp.float32, minval=-1.5, maxval=1.5)
    d_out = (jax.random.normal(key_list[5], (NUM_EXAMPLES, SEQ_LEN, D_MODEL), jnp.float32) * row_scale).astype(jnp.bfloat16)
    noise_up = jax.random.normal(key_list[6], (NUM_LAYERS, D_MODEL, D_FF), jnp.float32)
    noise_down = jax.random.normal(key_list[7], (NUM_LAYERS, D_FF, D_MODEL), jnp.float32)
    depth_pow = jnp.arange(NUM_LAYERS - 1, -1, -1).astype(jnp.float32)
    typical = math.sqrt(SEQ_LEN * D_MODEL * D_FF) * 1.2 ** depth_pow
    clip_up = typical * 0.335 * jax.random.uniform(key_list[8], (NUM_LAYERS,), jnp.float32, minval=0.2, maxval=0.5)
    clip_down = typical * 0.63 * jax.random.uniform(key_list[9], (NUM_LAYERS,), jnp.float32, minval=0.2, maxval=0.5)
    noise_mult = jax.random.uniform(key_list[10], (1,), jnp.float32, minval=0.25, maxval=0.6) * math.sqrt(NUM_EXAMPLES / (D_MODEL * D_FF))
    return {"x_stored": x_stored, "u_stored": u_stored, "w_up": w_up, "w_down": w_down, "d_out": d_out, "noise_up": noise_up, "noise_down": noise_down, "clip_up": clip_up, "clip_down": clip_down, "noise_mult": noise_mult}


def example_norms(x_layer, hidden, grad_z, grad_h):
    def one_example(example):
        x_row, h_row, dz_row, dh_row = example
        gram_x = jnp.dot(x_row, x_row.T, preferred_element_type=jnp.float32)
        gram_dh = jnp.dot(dh_row, dh_row.T, preferred_element_type=jnp.float32)
        gram_h = jnp.dot(h_row, h_row.T, preferred_element_type=jnp.float32)
        gram_dz = jnp.dot(dz_row, dz_row.T, preferred_element_type=jnp.float32)
        return jnp.stack([jnp.sum(gram_x * gram_dh), jnp.sum(gram_h * gram_dz)])
    return lax.map(one_example, (x_layer, hidden, grad_z, grad_h))


def reference(x_stored, u_stored, w_up, w_down, d_out, noise_up, noise_down, clip_up, clip_down, noise_mult):
    def layer_step(grad_z, layer_in):
        x_layer, u_layer, up_w, down_w, up_noise, down_noise, up_clip, down_clip = layer_in
        gelu_val, gelu_slope = gelu_pair(u_layer.astype(jnp.float32))
        hidden = gelu_val.astype(jnp.bfloat16)
        back_h = jnp.dot(grad_z.reshape(-1, D_MODEL), down_w.T, preferred_element_type=jnp.float32)
        grad_h = (gelu_slope * back_h.reshape(u_layer.shape)).astype(jnp.bfloat16)
        back_x = jnp.dot(grad_h.reshape(-1, D_FF), up_w.T, preferred_element_type=jnp.float32)
        next_z = (grad_z.astype(jnp.float32) + back_x.reshape(grad_z.shape)).astype(jnp.bfloat16)
        ghost_norms = example_norms(x_layer, hidden, grad_z, grad_h)
        scale_up = jnp.minimum(1.0, up_clip / jnp.sqrt(ghost_norms[:, 0]))
        scale_down = jnp.minimum(1.0, down_clip / jnp.sqrt(ghost_norms[:, 1]))
        dh_clip = (grad_h.astype(jnp.float32) * scale_up[:, None, None]).astype(jnp.bfloat16)
        dz_clip = (grad_z.astype(jnp.float32) * scale_down[:, None, None]).astype(jnp.bfloat16)
        sum_up = jnp.dot(x_layer.reshape(-1, D_MODEL).T, dh_clip.reshape(-1, D_FF), preferred_element_type=jnp.float32)
        sum_down = jnp.dot(hidden.reshape(-1, D_FF).T, dz_clip.reshape(-1, D_MODEL), preferred_element_type=jnp.float32)
        grad_up = (sum_up + noise_mult[0] * up_clip * up_noise) / NUM_EXAMPLES
        grad_down = (sum_down + noise_mult[0] * down_clip * down_noise) / NUM_EXAMPLES
        return next_z, (grad_up, grad_down)
    layer_inputs = (x_stored, u_stored, w_up, w_down, noise_up, noise_down, clip_up, clip_down)
    last_z, (grads_up, grads_down) = lax.scan(layer_step, d_out, layer_inputs, reverse=True)
    return grads_up, grads_down
```

```python
import math
import jax
import jax.numpy as jnp
from jax import lax
from jax.experimental import pallas as pl
from jax.experimental.pallas import tpu as pltpu
from jax.sharding import PartitionSpec as P


GELU_SCALE = math.sqrt(2.0 / math.pi)

T = 1024
D = 1024
Q = 1024
E = 4
TB = 512
NB = T // TB
KB = 512
GB = 256
F32 = jnp.float32
BF16 = jnp.bfloat16
ANY = pl.BlockSpec(memory_space=pl.ANY)
SMEM = pl.BlockSpec(memory_space=pltpu.SMEM)
TOKEN = jax.ShapeDtypeStruct((8, 128), F32)
TOKEN_SPEC = pl.BlockSpec((8, 128), lambda *_: (0, 0))
NT = (((1,), (1,)), ((), ()))
TN = (((0,), (0,)), ((), ()))
PARAMS = pltpu.CompilerParams(vmem_limit_bytes=63 * 1024 * 1024)


def gelu_pair(u):
    u2 = u * u
    t = jnp.tanh(u * (GELU_SCALE + (GELU_SCALE * 0.044715) * u2))
    half = 0.5 + 0.5 * t
    slope = half + (u * (1.0 - t * t)) * (0.5 * GELU_SCALE + (0.5 * GELU_SCALE * 0.134145) * u2)
    return u * half, slope


def block(i, size):
    return pl.ds(pl.multiple_of(i * size, size), size)


def gram_norms(x_ref, dz_ref, dh_ref, h_ref):
    def gram(ref, rows, cols):
        return lax.dot_general(ref[rows, :], ref[cols, :], NT, preferred_element_type=F32)

    def fold(p):
        return jnp.sum(p.reshape(p.shape[0] // 8, 8, GB), axis=0)

    def ring(k, sums):
        at = jnp.where(k == 3, 0, k)
        w = jnp.where(k == 3, 2.0, 1.0)
        rows, cols = pl.ds(pl.multiple_of(at * GB, GB), 2 * GB), block(k, GB)
        p1 = gram(x_ref, rows, cols) * gram(dh_ref, rows, cols)
        p2 = gram(h_ref, rows, cols) * gram(dz_ref, rows, cols)
        return tuple(t + (w * fold(p[:GB]) + 2.0 * fold(p[GB:])) for t, p in zip(sums, (p1, p2)))

    n1, n2 = lax.fori_loop(0, 4, ring, (jnp.zeros((8, GB), F32), jnp.zeros((8, GB), F32)))
    for r, c, w in ((3, 3, 1.0), (2, 0, 2.0)):
        rows, cols = slice(r * GB, (r + 1) * GB), slice(c * GB, (c + 1) * GB)
        n1 = n1 + w * fold(gram(x_ref, rows, cols) * gram(dh_ref, rows, cols))
        n2 = n2 + w * fold(gram(h_ref, rows, cols) * gram(dz_ref, rows, cols))
    return jnp.sum(n1), jnp.sum(n2)


def store_norms(n_ref, tok_ref, n1, n2):
    n_ref[0] = jnp.full((8, 128), n1, F32)
    n_ref[1] = jnp.full((8, 128), n2, F32)
    tok_ref[...] = jnp.zeros((8, 128), F32)


NORM_SHAPE = jax.ShapeDtypeStruct((E, 2, 8, 128), F32)


def norm_spec(ex):
    return pl.BlockSpec((None, 2, 8, 128), lambda *_: (ex, 0, 0, 0))


def chain_call(layer, ex, first, last, norms, scal, dz_prev, part_own, part_recv, u_all, u_recv, x_all, w_down, w_down_r, w_up, w_up_r, bufs, norm_buf, dep):
    at_u = ex if u_recv.shape[0] == E else (ex - 1 if u_recv.shape[0] > 1 else 0)
    at_w = layer if w_down_r.shape[0] > 1 else 0
    names = ["scal", "dz"]
    args = [scal, dz_prev]
    if not first:
        names += ["po", "pr"]
        args += [part_own, part_recv]
    names += ["uo", "ur", "w2o", "w2r"]
    args += [u_all, u_recv, w_down, w_down_r]
    if norms:
        names.append("x")
        args.append(x_all)
    if not last:
        names += ["w1o", "w1r"]
        args += [w_up, w_up_r]
    names.append("dep")
    args.append(dep)
    out_names = ["dz_out", "dh_out", "h_out", "tok"]
    out_shape = [jax.ShapeDtypeStruct((E, T, D), BF16), jax.ShapeDtypeStruct((E, T, 2 * Q), BF16), jax.ShapeDtypeStruct((E, T, 2 * Q), BF16), TOKEN]
    out_specs = [ANY, ANY, ANY, TOKEN_SPEC]
    aliases = {}
    if bufs is not None:
        for k, b in enumerate(bufs):
            aliases[len(args)] = k
            names.append(f"b{k}")
            args.append(b)
    if norms:
        if norm_buf is not None:
            aliases[len(args)] = len(out_names)
            names.append("bn")
            args.append(norm_buf)
        out_names.append("n_out")
        out_shape.append(NORM_SHAPE)
        out_specs.append(norm_spec(ex))
    if not last:
        out_names.append("part_out")
        out_shape.append(jax.ShapeDtypeStruct((T, D), BF16))
        out_specs.append(ANY)
    scratch = {
        "dzp": pltpu.VMEM((T, D), BF16), "po_s": pltpu.VMEM((T, D), BF16), "pr_s": pltpu.VMEM((T, D), BF16),
        "u_s": pltpu.VMEM((2, T, Q), BF16), "x_s": pltpu.VMEM((T, D), BF16), "w2_s": pltpu.VMEM((2 * Q, D), BF16), "w1_s": pltpu.VMEM((2, D, Q), BF16),
        "dz_s": pltpu.VMEM((T, D), BF16), "dh_s": pltpu.VMEM((T, 2 * Q), BF16), "h_s": pltpu.VMEM((T, 2 * Q), BF16), "part_s": pltpu.VMEM((T, D), BF16),
        "in_sem": pltpu.SemaphoreType.DMA((NB, 5)), "w_sem": pltpu.SemaphoreType.DMA((5,)), "out_sem": pltpu.SemaphoreType.DMA((NB, 4)),
    }

    def body(*refs):
        r = dict(zip(names + out_names + list(scratch), refs))
        here = r["scal"][0] * E + ex
        in_sem, w_sem, out_sem = r["in_sem"], r["w_sem"], r["out_sem"]
        dz_src = r["dz"].at[here] if first else r["dz"].at[ex]

        def inputs(i):
            rows = block(i, TB)
            copies = [pltpu.make_async_copy(dz_src.at[rows], r["dzp"].at[rows], in_sem.at[i, 0])]
            if not first:
                copies += [
                    pltpu.make_async_copy(r["po"].at[rows], r["po_s"].at[rows], in_sem.at[i, 1]),
                    pltpu.make_async_copy(r["pr"].at[rows], r["pr_s"].at[rows], in_sem.at[i, 2]),
                ]
            copies += [
                pltpu.make_async_copy(r["uo"].at[layer, here, rows], r["u_s"].at[0, rows], in_sem.at[i, 3]),
                pltpu.make_async_copy(r["ur"].at[at_u, rows], r["u_s"].at[1, rows], in_sem.at[i, 4]),
            ]
            return copies

        def outputs(i):
            rows = block(i, TB)
            return [
                pltpu.make_async_copy(r["dz_s"].at[rows], r["dz_out"].at[ex, rows], out_sem.at[i, 0]),
                pltpu.make_async_copy(r["dh_s"].at[rows], r["dh_out"].at[ex, rows], out_sem.at[i, 1]),
                pltpu.make_async_copy(r["h_s"].at[rows], r["h_out"].at[ex, rows], out_sem.at[i, 2]),
            ]

        def part_output(i):
            rows = block(i, TB)
            return pltpu.make_async_copy(r["part_s"].at[rows], r["part_out"].at[rows], out_sem.at[i, 3])

        w2 = [
            pltpu.make_async_copy(r["w2o"].at[layer], r["w2_s"].at[pl.ds(0, Q)], w_sem.at[0]),
            pltpu.make_async_copy(r["w2r"].at[at_w], r["w2_s"].at[pl.ds(Q, Q)], w_sem.at[1]),
        ]
        ins = inputs(0)
        for c in ins[:-2] + [w2[0], ins[-2], w2[1], ins[-1]]:
            c.start()
        if not last:
            w1 = [
                pltpu.make_async_copy(r["w1o"].at[layer], r["w1_s"].at[0], w_sem.at[2]),
                pltpu.make_async_copy(r["w1r"].at[at_w], r["w1_s"].at[1], w_sem.at[3]),
            ]
            for c in w1:
                c.start()
        for i in range(1, NB):
            for c in inputs(i):
                c.start()
        if norms:
            x_copy = pltpu.make_async_copy(r["x"].at[layer, here], r["x_s"], w_sem.at[4])
            x_copy.start()
        for c in w2:
            c.wait()

        def rows_step(i, carry):
            rows = block(i, TB)
            for c in inputs(i):
                c.wait()
            if first:
                dz = r["dzp"][rows, :]
            else:
                dz = (r["dzp"][rows, :].astype(F32) + (r["po_s"][rows, :].astype(F32) + r["pr_s"][rows, :].astype(F32))).astype(BF16)
            r["dz_s"][rows, :] = dz
            for c in range(4):
                cols = slice(c * 512, (c + 1) * 512)
                back = lax.dot_general(dz, r["w2_s"][cols, :], NT, preferred_element_type=F32)
                val, slope = gelu_pair(r["u_s"][c // 2, rows, (c % 2) * 512:(c % 2 + 1) * 512].astype(F32))
                r["dh_s"][rows, cols] = (slope * back).astype(BF16)
                r["h_s"][rows, cols] = val.astype(BF16)
            if not last:

                @pl.when(i == 0)
                def _():
                    for c in w1:
                        c.wait()

                for c in range(2):
                    cols = slice(c * 512, (c + 1) * 512)
                    acc = lax.dot_general(r["dh_s"][rows, :Q], r["w1_s"][0, cols, :], NT, preferred_element_type=F32)
                    acc = acc + lax.dot_general(r["dh_s"][rows, Q:], r["w1_s"][1, cols, :], NT, preferred_element_type=F32)
                    r["part_s"][rows, cols] = acc.astype(BF16)
            for c in outputs(i):
                c.start()
            if not last:
                part_output(i).start()
            return carry

        lax.fori_loop(0, NB, rows_step, 0)
        if norms:
            x_copy.wait()
            store_norms(r["n_out"], r["tok"], *gram_norms(r["x_s"], r["dz_s"], r["dh_s"], r["h_s"]))
        else:
            r["tok"][...] = jnp.zeros((8, 128), F32)
        for i in range(NB):
            for c in outputs(i):
                c.wait()
            if not last:
                part_output(i).wait()

    outs = pl.pallas_call(
        body,
        out_shape=out_shape,
        in_specs=[SMEM] + [ANY] * (len(args) - 1),
        out_specs=out_specs,
        scratch_shapes=list(scratch.values()),
        input_output_aliases=aliases,
        compiler_params=PARAMS,
        grid=(1,),
    )(*args)
    named = dict(zip(out_names, outs))
    return outs[:3], named.get("n_out", norm_buf), named.get("part_out"), named["tok"]


def norm_call(layer, ex, scal, x_all, bufs, dep):
    def body(s_ref, x_ref, dz_ref, dh_ref, h_ref, dep_ref, n_ref, tok_ref):
        store_norms(n_ref, tok_ref, *gram_norms(x_ref, dz_ref, dh_ref, h_ref))

    def at(width):
        return pl.BlockSpec((None, T, width), lambda i, s: (ex, 0, 0))

    return pl.pallas_call(
        body,
        out_shape=[NORM_SHAPE, TOKEN],
        grid_spec=pltpu.PrefetchScalarGridSpec(
            num_scalar_prefetch=1, grid=(1,),
            in_specs=[pl.BlockSpec((None, None, T, D), lambda i, s: (layer, s[0] * E + ex, 0, 0)), at(D), at(2 * Q), at(2 * Q), ANY],
            out_specs=[norm_spec(ex), TOKEN_SPEC],
        ),
        compiler_params=PARAMS,
    )(scal, x_all, *bufs, dep)


def weight_call(layer, half, x_all, bufs, norms, norms_recv, clip_up, clip_down, scal, recv, dep):
    dz, dh, hid = bufs
    own = half == 0
    steps = E * T // KB
    per = T // KB

    def body(*refs):
        refs = list(refs)
        s_ref, x_ref, dh_ref, h_ref, dz_ref, no_ref, nr_ref, cu_ref, cd_ref = refs[:9]
        del refs[:9]
        if own:
            recv_ref = refs.pop(0)
        refs.pop(0)
        if own:
            send_ref, keep_ref, tok_ref, acc, recv_s, sem, recv_sem = refs
        else:
            g_ref, tok_ref, acc, sem = refs
        k = pl.program_id(0)
        n = no_ref[...] + nr_ref[...]
        c1 = jnp.minimum(1.0, cu_ref[layer] / jnp.sqrt(n[0, 0:1, 0:1]))
        c2 = jnp.minimum(1.0, cd_ref[layer] / jnp.sqrt(n[1, 0:1, 0:1]))
        y = s_ref[1]
        halves = (1 - y, y) if own else (0, 1)
        if own:
            recv_copy = pltpu.make_async_copy(recv_ref, recv_s, recv_sem)

        def copies(g, at):
            ds = block(halves[at], 512)
            if not own:
                part = (0, ds) if g == 0 else (1, slice(None), ds)
                return [pltpu.make_async_copy(acc.at[part], g_ref.at[part], sem.at[g, at, 0])]
            out = (send_ref, keep_ref)[at]
            if g == 0:
                return [pltpu.make_async_copy(acc.at[0, ds], out.at[0], sem.at[g, at, 0])]
            return [
                pltpu.make_async_copy(acc.at[1, pl.ds(b * 512, 512), ds], out.at[1, :, pl.ds(b * 512, 512)], sem.at[g, at, b])
                for b in range(2)
            ]

        @pl.when(k == 0)
        def _():
            tok_ref[...] = jnp.zeros((8, 128), F32)
            if own:
                recv_copy.start()

        def add(init, final):
            dhc = (dh_ref[...].astype(F32) * c1).astype(BF16)
            if final and own:
                recv_copy.wait()
            started = []
            for at in range(2):
                ds = block(halves[at], 512)
                for g in range(2):
                    if g == 0:
                        part = (0, ds)
                        new = lax.dot_general(x_ref[:, ds], dhc, TN, preferred_element_type=F32)
                    else:
                        part = (1, slice(None), ds)
                        new = lax.dot_general(h_ref[...], (dz_ref[:, ds].astype(F32) * c2).astype(BF16), TN, preferred_element_type=F32)
                    if not init:
                        new = acc[part] + new
                    if final and own:
                        new = new + recv_s[part]
                    acc[part] = new
                    if final:
                        if started:
                            for c in copies(*started[-1]):
                                c.start()
                        started.append((g, at))
            if final:
                for c in copies(*started[-1]):
                    c.start()
                for s in started:
                    for c in copies(*s):
                        c.wait()

        @pl.when(k == 0)
        def _():
            add(True, False)

        @pl.when((k > 0) & (k < steps - 1))
        def _():
            add(False, False)

        @pl.when(k == steps - 1)
        def _():
            add(False, True)

    norm_in = pl.BlockSpec((None, 2, 8, 128), lambda k, s: (k // per, 0, 0, 0))
    in_specs = [
        pl.BlockSpec((None, None, KB, D), lambda k, s: (layer, s[0] * E + k // per, k % per, 0)),
        pl.BlockSpec((None, KB, Q), lambda k, s: (k // per, k % per, half)),
        pl.BlockSpec((None, KB, Q), lambda k, s: (k // per, k % per, half)),
        pl.BlockSpec((None, KB, D), lambda k, s: (k // per, k % per, 0)),
        norm_in, norm_in, SMEM, SMEM,
    ]
    args = [x_all, dh, hid, dz, norms, norms_recv, clip_up, clip_down]
    piece = jax.ShapeDtypeStruct((2, 512, 1024), F32)
    scratch = [pltpu.VMEM((2, 1024, 1024), F32)]
    if own:
        in_specs.append(ANY)
        args.append(recv)
        out_shape, out_specs = [piece, piece, TOKEN], [ANY, ANY, TOKEN_SPEC]
        scratch += [pltpu.VMEM((2, 1024, 1024), F32), pltpu.SemaphoreType.DMA((2, 2, 2)), pltpu.SemaphoreType.DMA]
    else:
        out_shape, out_specs = [jax.ShapeDtypeStruct((2, 1024, 1024), F32), TOKEN], [ANY, TOKEN_SPEC]
        scratch += [pltpu.SemaphoreType.DMA((2, 2, 2))]
    return pl.pallas_call(
        body,
        out_shape=out_shape,
        grid_spec=pltpu.PrefetchScalarGridSpec(
            num_scalar_prefetch=1, grid=(steps,), in_specs=in_specs + [ANY], out_specs=out_specs, scratch_shapes=scratch,
        ),
        compiler_params=PARAMS,
    )(scal, *args, dep)


def pack_call(layer, start, count, scal, u_all, dep, weights=()):
    nw = len(weights)

    def body(*refs):
        ins, outs = refs[1:2 + nw], refs[3 + nw:4 + 2 * nw]
        for a, b in zip(ins, outs):
            b[...] = a[...]
        refs[-1][...] = jnp.zeros((8, 128), F32)

    w_in = pl.BlockSpec((None, 512, 1024), lambda e, i, s: (layer, i, 0))
    w_out = pl.BlockSpec((None, 512, 1024), lambda e, i, s: (0, i, 0))
    return pl.pallas_call(
        body,
        out_shape=[jax.ShapeDtypeStruct((count, T, Q), BF16)] + [jax.ShapeDtypeStruct((1, 1024, 1024), BF16)] * nw + [TOKEN],
        grid_spec=pltpu.PrefetchScalarGridSpec(
            num_scalar_prefetch=1, grid=(count, 2),
            in_specs=[pl.BlockSpec((None, None, 512, Q), lambda e, i, s: (layer, (1 - s[0]) * E + start + e, i, 0))] + [w_in] * nw + [ANY],
            out_specs=[pl.BlockSpec((None, 512, Q), lambda e, i, s: (e, i, 0))] + [w_out] * nw + [TOKEN_SPEC],
        ),
        compiler_params=PARAMS,
    )(scal, u_all, *weights, dep)


def final_call(layer, num_layers, total, keep, y_recv, noise_up, noise_down, clip_up, clip_down, noise_mult, outs, dep):
    def body(*refs):
        k1, k2, y1, y2, n1, n2, cu, cd, sg = refs[:9]
        up, down, tok_ref = refs[-3:]
        up[...] = (k1[...] + y1[...] + (sg[0] * cu[layer]) * n1[...]) / total
        down[...] = (k2[...] + y2[...] + (sg[0] * cd[layer]) * n2[...]) / total
        tok_ref[...] = jnp.zeros((8, 128), F32)

    s1 = pl.BlockSpec((None, 512, 512), lambda j: (0, 0, j))
    s2 = pl.BlockSpec((None, 512, 512), lambda j: (1, 0, j))
    up_spec = pl.BlockSpec((None, 512, 512), lambda j: (layer, 0, j))
    down_spec = pl.BlockSpec((None, 512, 512), lambda j: (layer, j, 0))
    in_specs = [s1, s2, s1, s2, up_spec, down_spec, SMEM, SMEM, SMEM, ANY]
    args = [keep, keep, y_recv, y_recv, noise_up, noise_down, clip_up, clip_down, noise_mult, dep]
    aliases = {}
    if outs is not None:
        in_specs += [ANY, ANY]
        args += list(outs)
        aliases = {10: 0, 11: 1}
    up, down, tok = pl.pallas_call(
        body,
        out_shape=[jax.ShapeDtypeStruct((num_layers, 512, 1024), F32), jax.ShapeDtypeStruct((num_layers, 1024, 512), F32), TOKEN],
        grid=(2,),
        in_specs=in_specs,
        out_specs=[up_spec, down_spec, TOKEN_SPEC],
        input_output_aliases=aliases,
        compiler_params=PARAMS,
    )(*args)
    return (up, down), tok


def program_order(num_layers):
    top = num_layers - 1
    order = [("k", "pack", top, 0), ("p", "u", top, 0), ("p", "w", top, 0), ("p", "w", top, 1)]
    order += [("k", "pack", top, 1), ("p", "u", top, 1), ("p", "w", 0, 0), ("p", "w", 0, 1)]

    def chain(layer, e):
        steps = [("k", "chain", layer, e)]
        if e == E - 1:
            steps.append(("p", "n", layer, 0))
        if layer > 0:
            steps.append(("p", "x", layer, e))
        if layer == top and e == 0:
            steps.append(("k", "norm", layer, e))
        return steps

    def give(layer):
        return [("k", "wgrad", layer, 1), ("p", "c", layer, 0)]

    def own(layer):
        return [("k", "wgrad", layer, 0), ("p", "y", layer, 0)]

    for layer in reversed(range(num_layers)):
        order += chain(layer, 0)
        if layer > 0:
            order += [("k", "pack", layer - 1, E), ("p", "u", layer - 1, E)]
        order += chain(layer, 1)
        if layer + 2 <= top:
            order.append(("k", "final", layer + 2, 0))
        order += chain(layer, 2)
        if layer + 1 <= top:
            order += give(layer + 1)
        if layer > 0:
            order += chain(layer, 3)
            if layer + 1 <= top:
                order += own(layer + 1)
        else:
            order += own(1) + chain(0, 3)
    order += give(0) + own(0)
    order += [("k", "final", 1, 0), ("k", "final", 0, 0)]
    return order


def solution(mesh):
    in_specs = (P(None, "dp", None, None), P(None, "dp", None, "tp"), P(None, None, "tp"), P(None, "tp", None), P("dp", None, None), P(None, "dp", "tp"), P(None, "tp", "dp"), P(), P(), P())
    out_specs = (P(None, "dp", "tp"), P(None, "tp", "dp"))
    swap_core = [(0, 1), (1, 0), (2, 3), (3, 2)]
    swap_x = [(0, 2), (2, 0), (1, 3), (3, 1)]
    swap_dp = [(0, 1), (1, 0)]
    num_layers = 6

    def local_step(x_stored, u_stored, w_up, w_down, d_out, noise_up, noise_down, clip_up, clip_down, noise_mult):
        total = float(d_out.shape[0] * mesh.shape["dp"])
        top = num_layers - 1
        scal = jnp.stack([lax.axis_index("tp") % 2, lax.axis_index("dp")]).astype(jnp.int32)
        tok = jnp.zeros((8, 128), F32)
        bufs, norms, part, part_recv, packed, u_recv, w_pack, w_recv = {}, {}, {}, {}, {}, {}, {}, {}
        norms_recv, give, recv, y_send, keep, y_recv = {}, {}, {}, {}, {}, {}
        outs = None
        for step in program_order(num_layers):
            kind, what, layer, k = step
            first, last = layer == top, layer == 0
            if kind == "p":
                if what == "u":
                    u_recv[layer, k] = lax.ppermute(packed[layer, k], "tp", swap_core)
                elif what == "w":
                    w_recv[layer, k] = lax.ppermute(w_pack[k] if first else (w_down, w_up)[k], "tp", swap_core)
                elif what == "n":
                    norms_recv[layer] = lax.ppermute(norms[layer], "tp", swap_x)
                elif what == "x":
                    part_recv[layer, k] = lax.ppermute(part[layer, k], "tp", swap_x)
                elif what == "c":
                    recv[layer] = lax.ppermute(give[layer], "tp", swap_core)
                else:
                    y_recv[layer] = lax.ppermute(y_send[layer], "dp", swap_dp)
            elif what == "pack":
                if first and k == 0:
                    packed[layer, k], w_pack[0], w_pack[1], tok = pack_call(layer, 0, 1, scal, u_stored, tok, (w_down, w_up))
                elif first:
                    packed[layer, k], tok = pack_call(layer, 1, E - 1, scal, u_stored, tok)
                else:
                    packed[layer, k], tok = pack_call(layer, 0, E, scal, u_stored, tok)
            elif what == "chain":
                w_at = top if first else 0
                bufs[layer], norms[layer], part[layer, k], tok = chain_call(
                    layer, k, first, last, not (first and k == 0), scal,
                    d_out if first else bufs[layer + 1][0], None if first else part[layer + 1, k], None if first else part_recv[layer + 1, k],
                    u_stored, u_recv[layer, min(k, 1) if first else E], x_stored,
                    w_down, w_recv[w_at, 0], w_up, w_recv[w_at, 1], bufs.get(layer), norms.get(layer), tok,
                )
            elif what == "norm":
                norms[layer], tok = norm_call(layer, k, scal, x_stored, bufs[layer], tok)
            elif what == "wgrad":
                got = weight_call(
                    layer, k, x_stored, bufs[layer], norms[layer], norms_recv[layer], clip_up, clip_down, scal, recv.get(layer), tok
                )
                tok = got[-1]
                if k == 1:
                    give[layer] = got[0]
                else:
                    y_send[layer], keep[layer] = got[:2]
            else:
                outs, tok = final_call(
                    layer, num_layers, total, keep[layer], y_recv[layer], noise_up, noise_down, clip_up, clip_down, noise_mult, outs, tok
                )
        return outs

    return jax.shard_map(local_step, mesh=mesh, in_specs=in_specs, out_specs=out_specs, check_vma=False)
```

```python
import math
import jax
import jax.numpy as jnp
from jax import lax
from jax.experimental import pallas as pl
from jax.experimental.pallas import tpu as pltpu
from jax.sharding import PartitionSpec as P


GELU_SCALE = math.sqrt(2.0 / math.pi)

T = 1024
D = 1024
Q = 1024
E = 4
TB = 512
NB = T // TB
KB = 512
GB = 256
F32 = jnp.float32
BF16 = jnp.bfloat16
ANY = pl.BlockSpec(memory_space=pl.ANY)
SMEM = pl.BlockSpec(memory_space=pltpu.SMEM)
TOKEN = jax.ShapeDtypeStruct((8, 128), F32)
TOKEN_SPEC = pl.BlockSpec((8, 128), lambda *_: (0, 0))
NT = (((1,), (1,)), ((), ()))
TN = (((0,), (0,)), ((), ()))
PARAMS = pltpu.CompilerParams(vmem_limit_bytes=63 * 1024 * 1024)


def gelu_pair(u):
    u2 = u * u
    t = jnp.tanh(u * (GELU_SCALE + (GELU_SCALE * 0.044715) * u2))
    half = 0.5 + 0.5 * t
    slope = half + (u * (1.0 - t * t)) * (0.5 * GELU_SCALE + (0.5 * GELU_SCALE * 0.134145) * u2)
    return u * half, slope


def block(i, size):
    return pl.ds(pl.multiple_of(i * size, size), size)


def gram_norms(x_ref, dz_ref, dh_ref, h_ref):
    def gram(ref, rows, cols):
        return lax.dot_general(ref[rows, :], ref[cols, :], NT, preferred_element_type=F32)

    def fold(p):
        return jnp.sum(p.reshape(p.shape[0] // 8, 8, GB), axis=0)

    def ring(k, sums):
        at = jnp.where(k == 3, 0, k)
        w = jnp.where(k == 3, 2.0, 1.0)
        rows, cols = pl.ds(pl.multiple_of(at * GB, GB), 2 * GB), block(k, GB)
        p1 = gram(x_ref, rows, cols) * gram(dh_ref, rows, cols)
        p2 = gram(h_ref, rows, cols) * gram(dz_ref, rows, cols)
        return tuple(t + (w * fold(p[:GB]) + 2.0 * fold(p[GB:])) for t, p in zip(sums, (p1, p2)))

    n1, n2 = lax.fori_loop(0, 4, ring, (jnp.zeros((8, GB), F32), jnp.zeros((8, GB), F32)))
    for r, c, w in ((3, 3, 1.0), (2, 0, 2.0)):
        rows, cols = slice(r * GB, (r + 1) * GB), slice(c * GB, (c + 1) * GB)
        n1 = n1 + w * fold(gram(x_ref, rows, cols) * gram(dh_ref, rows, cols))
        n2 = n2 + w * fold(gram(h_ref, rows, cols) * gram(dz_ref, rows, cols))
    return jnp.sum(n1), jnp.sum(n2)


def store_norms(n_ref, tok_ref, n1, n2):
    n_ref[0] = jnp.full((8, 128), n1, F32)
    n_ref[1] = jnp.full((8, 128), n2, F32)
    tok_ref[...] = jnp.zeros((8, 128), F32)


NORM_SHAPE = jax.ShapeDtypeStruct((E, 2, 8, 128), F32)


def norm_spec(ex):
    return pl.BlockSpec((None, 2, 8, 128), lambda *_: (ex, 0, 0, 0))


def chain_call(layer, ex, first, last, norms, scal, dz_prev, part_own, part_recv, u_all, u_recv, x_all, w_down, w_down_r, w_up, w_up_r, bufs, norm_buf, pack_buf, dep):
    packs = not last and ex < 2
    at_u = ex if u_recv.shape[0] == E else (ex - 1 if u_recv.shape[0] > 1 else 0)
    at_w = layer if w_down_r.shape[0] > 1 else 0
    names = ["scal", "dz"]
    args = [scal, dz_prev]
    if not first:
        names += ["po", "pr"]
        args += [part_own, part_recv]
    names += ["uo", "ur", "w2o", "w2r"]
    args += [u_all, u_recv, w_down, w_down_r]
    if norms:
        names.append("x")
        args.append(x_all)
    if not last:
        names += ["w1o", "w1r"]
        args += [w_up, w_up_r]
    names.append("dep")
    args.append(dep)
    out_names = ["dz_out", "dh_out", "h_out", "tok"]
    out_shape = [jax.ShapeDtypeStruct((E, T, D), BF16), jax.ShapeDtypeStruct((E, T, 2 * Q), BF16), jax.ShapeDtypeStruct((E, T, 2 * Q), BF16), TOKEN]
    out_specs = [ANY, ANY, ANY, TOKEN_SPEC]
    aliases = {}
    if bufs is not None:
        for k, b in enumerate(bufs):
            aliases[len(args)] = k
            names.append(f"b{k}")
            args.append(b)
    if norms:
        if norm_buf is not None:
            aliases[len(args)] = len(out_names)
            names.append("bn")
            args.append(norm_buf)
        out_names.append("n_out")
        out_shape.append(NORM_SHAPE)
        out_specs.append(norm_spec(ex))
    if not last:
        out_names.append("part_out")
        out_shape.append(jax.ShapeDtypeStruct((T, D), BF16))
        out_specs.append(ANY)
    if packs:
        if pack_buf is not None:
            aliases[len(args)] = len(out_names)
            names.append("bp")
            args.append(pack_buf)
        out_names.append("pack_out")
        out_shape.append(jax.ShapeDtypeStruct((E, T, Q), BF16))
        out_specs.append(ANY)
    scratch = {
        "dzp": pltpu.VMEM((T, D), BF16), "po_s": pltpu.VMEM((T, D), BF16), "pr_s": pltpu.VMEM((T, D), BF16),
        "u_s": pltpu.VMEM((2, T, Q), BF16), "x_s": pltpu.VMEM((T, D), BF16), "w2_s": pltpu.VMEM((2 * Q, D), BF16), "w1_s": pltpu.VMEM((2, D, Q), BF16),
        "dz_s": pltpu.VMEM((T, D), BF16), "dh_s": pltpu.VMEM((T, 2 * Q), BF16), "h_s": pltpu.VMEM((T, 2 * Q), BF16), "part_s": pltpu.VMEM((T, D), BF16),
        "in_sem": pltpu.SemaphoreType.DMA((NB, 5)), "w_sem": pltpu.SemaphoreType.DMA((5,)), "out_sem": pltpu.SemaphoreType.DMA((NB, 4)),
        "pk_s": pltpu.VMEM((2, T, Q), BF16), "pk_sem": pltpu.SemaphoreType.DMA((2, 2)),
    }

    def body(*refs):
        r = dict(zip(names + out_names + list(scratch), refs))
        here = r["scal"][0] * E + ex
        in_sem, w_sem, out_sem = r["in_sem"], r["w_sem"], r["out_sem"]
        dz_src = r["dz"].at[here] if first else r["dz"].at[ex]

        def inputs(i):
            rows = block(i, TB)
            copies = [pltpu.make_async_copy(dz_src.at[rows], r["dzp"].at[rows], in_sem.at[i, 0])]
            if not first:
                copies += [
                    pltpu.make_async_copy(r["po"].at[rows], r["po_s"].at[rows], in_sem.at[i, 1]),
                    pltpu.make_async_copy(r["pr"].at[rows], r["pr_s"].at[rows], in_sem.at[i, 2]),
                ]
            copies += [
                pltpu.make_async_copy(r["uo"].at[layer, here, rows], r["u_s"].at[0, rows], in_sem.at[i, 3]),
                pltpu.make_async_copy(r["ur"].at[at_u, rows], r["u_s"].at[1, rows], in_sem.at[i, 4]),
            ]
            return copies

        def outputs(i):
            rows = block(i, TB)
            return [
                pltpu.make_async_copy(r["dz_s"].at[rows], r["dz_out"].at[ex, rows], out_sem.at[i, 0]),
                pltpu.make_async_copy(r["dh_s"].at[rows], r["dh_out"].at[ex, rows], out_sem.at[i, 1]),
                pltpu.make_async_copy(r["h_s"].at[rows], r["h_out"].at[ex, rows], out_sem.at[i, 2]),
            ]

        def part_output(i):
            rows = block(i, TB)
            return pltpu.make_async_copy(r["part_s"].at[rows], r["part_out"].at[rows], out_sem.at[i, 3])

        w2 = [
            pltpu.make_async_copy(r["w2o"].at[layer], r["w2_s"].at[pl.ds(0, Q)], w_sem.at[0]),
            pltpu.make_async_copy(r["w2r"].at[at_w], r["w2_s"].at[pl.ds(Q, Q)], w_sem.at[1]),
        ]
        ins = inputs(0)
        for c in ins[:-2] + [w2[0], ins[-2], w2[1], ins[-1]]:
            c.start()
        if not last:
            w1 = [
                pltpu.make_async_copy(r["w1o"].at[layer], r["w1_s"].at[0], w_sem.at[2]),
                pltpu.make_async_copy(r["w1r"].at[at_w], r["w1_s"].at[1], w_sem.at[3]),
            ]
            for c in w1:
                c.start()
        for i in range(1, NB):
            for c in inputs(i):
                c.start()
        if norms:
            x_copy = pltpu.make_async_copy(r["x"].at[layer, here], r["x_s"], w_sem.at[4])
            x_copy.start()
        if packs:
            there = (1 - r["scal"][0]) * E
            pack_in = [pltpu.make_async_copy(r["uo"].at[layer - 1, there + 2 * ex + j], r["pk_s"].at[j], r["pk_sem"].at[0, j]) for j in range(2)]
            pack_out = [pltpu.make_async_copy(r["pk_s"].at[j], r["pack_out"].at[2 * ex + j], r["pk_sem"].at[1, j]) for j in range(2)]
            for c in pack_in:
                c.start()
        for c in w2:
            c.wait()

        def rows_step(i, carry):
            rows = block(i, TB)
            for c in inputs(i):
                c.wait()
            if first:
                dz = r["dzp"][rows, :]
            else:
                dz = (r["dzp"][rows, :].astype(F32) + (r["po_s"][rows, :].astype(F32) + r["pr_s"][rows, :].astype(F32))).astype(BF16)
            r["dz_s"][rows, :] = dz
            for c in range(4):
                cols = slice(c * 512, (c + 1) * 512)
                back = lax.dot_general(dz, r["w2_s"][cols, :], NT, preferred_element_type=F32)
                val, slope = gelu_pair(r["u_s"][c // 2, rows, (c % 2) * 512:(c % 2 + 1) * 512].astype(F32))
                r["dh_s"][rows, cols] = (slope * back).astype(BF16)
                r["h_s"][rows, cols] = val.astype(BF16)
            if not last:

                @pl.when(i == 0)
                def _():
                    for c in w1:
                        c.wait()

                for c in range(2):
                    cols = slice(c * 512, (c + 1) * 512)
                    acc = lax.dot_general(r["dh_s"][rows, :Q], r["w1_s"][0, cols, :], NT, preferred_element_type=F32)
                    acc = acc + lax.dot_general(r["dh_s"][rows, Q:], r["w1_s"][1, cols, :], NT, preferred_element_type=F32)
                    r["part_s"][rows, cols] = acc.astype(BF16)
            for c in outputs(i):
                c.start()
            if not last:
                part_output(i).start()
            return carry

        lax.fori_loop(0, NB, rows_step, 0)
        if packs:
            for a, b in zip(pack_in, pack_out):
                a.wait()
                b.start()
        if norms:
            x_copy.wait()
            store_norms(r["n_out"], r["tok"], *gram_norms(r["x_s"], r["dz_s"], r["dh_s"], r["h_s"]))
        else:
            r["tok"][...] = jnp.zeros((8, 128), F32)
        for i in range(NB):
            for c in outputs(i):
                c.wait()
            if not last:
                part_output(i).wait()
        if packs:
            for b in pack_out:
                b.wait()

    outs = pl.pallas_call(
        body,
        out_shape=out_shape,
        in_specs=[SMEM] + [ANY] * (len(args) - 1),
        out_specs=out_specs,
        scratch_shapes=list(scratch.values()),
        input_output_aliases=aliases,
        compiler_params=PARAMS,
        grid=(1,),
    )(*args)
    named = dict(zip(out_names, outs))
    return outs[:3], named.get("n_out", norm_buf), named.get("part_out"), named.get("pack_out", pack_buf), named["tok"]


def norm_call(layer, ex, scal, x_all, bufs, dep):
    def body(s_ref, x_ref, dz_ref, dh_ref, h_ref, dep_ref, n_ref, tok_ref):
        store_norms(n_ref, tok_ref, *gram_norms(x_ref, dz_ref, dh_ref, h_ref))

    def at(width):
        return pl.BlockSpec((None, T, width), lambda i, s: (ex, 0, 0))

    return pl.pallas_call(
        body,
        out_shape=[NORM_SHAPE, TOKEN],
        grid_spec=pltpu.PrefetchScalarGridSpec(
            num_scalar_prefetch=1, grid=(1,),
            in_specs=[pl.BlockSpec((None, None, T, D), lambda i, s: (layer, s[0] * E + ex, 0, 0)), at(D), at(2 * Q), at(2 * Q), ANY],
            out_specs=[norm_spec(ex), TOKEN_SPEC],
        ),
        compiler_params=PARAMS,
    )(scal, x_all, *bufs, dep)


def weight_call(layer, half, x_all, bufs, norms, norms_recv, clip_up, clip_down, scal, recv, dep):
    dz, dh, hid = bufs
    own = half == 0
    steps = E * T // KB
    per = T // KB

    def body(*refs):
        refs = list(refs)
        s_ref, x_ref, dh_ref, h_ref, dz_ref, no_ref, nr_ref, cu_ref, cd_ref = refs[:9]
        del refs[:9]
        if own:
            recv_ref = refs.pop(0)
        refs.pop(0)
        if own:
            send_ref, keep_ref, tok_ref, acc, recv_s, sem, recv_sem = refs
        else:
            g_ref, tok_ref, acc, sem = refs
        k = pl.program_id(0)
        n = no_ref[...] + nr_ref[...]
        c1 = jnp.minimum(1.0, cu_ref[layer] / jnp.sqrt(n[0, 0:1, 0:1]))
        c2 = jnp.minimum(1.0, cd_ref[layer] / jnp.sqrt(n[1, 0:1, 0:1]))
        y = s_ref[1]
        halves = (1 - y, y) if own else (0, 1)
        if own:
            recv_copy = pltpu.make_async_copy(recv_ref, recv_s, recv_sem)

        def copies(g, at):
            ds = block(halves[at], 512)
            if not own:
                part = (0, ds) if g == 0 else (1, slice(None), ds)
                return [pltpu.make_async_copy(acc.at[part], g_ref.at[part], sem.at[g, at, 0])]
            out = (send_ref, keep_ref)[at]
            if g == 0:
                return [pltpu.make_async_copy(acc.at[0, ds], out.at[0], sem.at[g, at, 0])]
            return [
                pltpu.make_async_copy(acc.at[1, pl.ds(b * 512, 512), ds], out.at[1, :, pl.ds(b * 512, 512)], sem.at[g, at, b])
                for b in range(2)
            ]

        @pl.when(k == 0)
        def _():
            tok_ref[...] = jnp.zeros((8, 128), F32)
            if own:
                recv_copy.start()

        def add(init, final):
            dhc = (dh_ref[...].astype(F32) * c1).astype(BF16)
            if final and own:
                recv_copy.wait()
            started = []
            for at in range(2):
                ds = block(halves[at], 512)
                for g in range(2):
                    if g == 0:
                        part = (0, ds)
                        new = lax.dot_general(x_ref[:, ds], dhc, TN, preferred_element_type=F32)
                    else:
                        part = (1, slice(None), ds)
                        new = lax.dot_general(h_ref[...], (dz_ref[:, ds].astype(F32) * c2).astype(BF16), TN, preferred_element_type=F32)
                    if not init:
                        new = acc[part] + new
                    if final and own:
                        new = new + recv_s[part]
                    acc[part] = new
                    if final:
                        if started:
                            for c in copies(*started[-1]):
                                c.start()
                        started.append((g, at))
            if final:
                for c in copies(*started[-1]):
                    c.start()
                for s in started:
                    for c in copies(*s):
                        c.wait()

        @pl.when(k == 0)
        def _():
            add(True, False)

        @pl.when((k > 0) & (k < steps - 1))
        def _():
            add(False, False)

        @pl.when(k == steps - 1)
        def _():
            add(False, True)

    norm_in = pl.BlockSpec((None, 2, 8, 128), lambda k, s: (k // per, 0, 0, 0))
    in_specs = [
        pl.BlockSpec((None, None, KB, D), lambda k, s: (layer, s[0] * E + k // per, k % per, 0)),
        pl.BlockSpec((None, KB, Q), lambda k, s: (k // per, k % per, half)),
        pl.BlockSpec((None, KB, Q), lambda k, s: (k // per, k % per, half)),
        pl.BlockSpec((None, KB, D), lambda k, s: (k // per, k % per, 0)),
        norm_in, norm_in, SMEM, SMEM,
    ]
    args = [x_all, dh, hid, dz, norms, norms_recv, clip_up, clip_down]
    piece = jax.ShapeDtypeStruct((2, 512, 1024), F32)
    scratch = [pltpu.VMEM((2, 1024, 1024), F32)]
    if own:
        in_specs.append(ANY)
        args.append(recv)
        out_shape, out_specs = [piece, piece, TOKEN], [ANY, ANY, TOKEN_SPEC]
        scratch += [pltpu.VMEM((2, 1024, 1024), F32), pltpu.SemaphoreType.DMA((2, 2, 2)), pltpu.SemaphoreType.DMA]
    else:
        out_shape, out_specs = [jax.ShapeDtypeStruct((2, 1024, 1024), F32), TOKEN], [ANY, TOKEN_SPEC]
        scratch += [pltpu.SemaphoreType.DMA((2, 2, 2))]
    return pl.pallas_call(
        body,
        out_shape=out_shape,
        grid_spec=pltpu.PrefetchScalarGridSpec(
            num_scalar_prefetch=1, grid=(steps,), in_specs=in_specs + [ANY], out_specs=out_specs, scratch_shapes=scratch,
        ),
        compiler_params=PARAMS,
    )(scal, *args, dep)


def weight_piece_call(layer, half, at, x_all, bufs, norms, norms_recv, clip_up, clip_down, scal, recv, dep):
    dz, dh, hid = bufs
    own = half == 0
    steps = E * T // KB
    per = T // KB

    def body(*refs):
        refs = list(refs)
        _, x_ref, dh_ref, h_ref, dz_ref, no_ref, nr_ref, cu_ref, cd_ref = refs[:9]
        del refs[:9]
        if own:
            recv_ref = refs.pop(0)
        refs.pop(0)
        out_ref, tok_ref, acc1, acc2 = refs
        k = pl.program_id(0)
        n = no_ref[...] + nr_ref[...]
        c1 = jnp.minimum(1.0, cu_ref[layer] / jnp.sqrt(n[0, 0:1, 0:1]))
        c2 = jnp.minimum(1.0, cd_ref[layer] / jnp.sqrt(n[1, 0:1, 0:1]))

        def products():
            g1 = lax.dot_general(x_ref[...], (dh_ref[...].astype(F32) * c1).astype(BF16), TN, preferred_element_type=F32)
            g2 = lax.dot_general(h_ref[...], (dz_ref[...].astype(F32) * c2).astype(BF16), TN, preferred_element_type=F32)
            return g1, g2

        @pl.when(k == 0)
        def _():
            tok_ref[...] = jnp.zeros((8, 128), F32)
            acc1[...], acc2[...] = products()

        @pl.when((k > 0) & (k < steps - 1))
        def _():
            g1, g2 = products()
            acc1[...] += g1
            acc2[...] += g2

        @pl.when(k == steps - 1)
        def _():
            g1, g2 = products()
            g1 = acc1[...] + g1
            g2 = acc2[...] + g2
            if own:
                g1 = g1 + recv_ref[0]
            out_ref[0] = g1
            for b in range(2):
                cols = slice(b * 512, (b + 1) * 512)
                out_ref[1, :, cols] = g2[cols] + recv_ref[1, :, cols] if own else g2[cols]

    def d_half(s):
        return 1 - s[1] if at == 0 else s[1]

    norm_in = pl.BlockSpec((None, 2, 8, 128), lambda k, s: (k // per, 0, 0, 0))
    piece = pl.BlockSpec((2, 512, 1024), lambda k, s: (0, 0, 0))
    in_specs = [
        pl.BlockSpec((None, None, KB, 512), lambda k, s: (layer, s[0] * E + k // per, k % per, d_half(s))),
        pl.BlockSpec((None, KB, Q), lambda k, s: (k // per, k % per, half)),
        pl.BlockSpec((None, KB, Q), lambda k, s: (k // per, k % per, half)),
        pl.BlockSpec((None, KB, 512), lambda k, s: (k // per, k % per, d_half(s))),
        norm_in, norm_in, SMEM, SMEM,
    ]
    args = [x_all, dh, hid, dz, norms, norms_recv, clip_up, clip_down]
    if own:
        in_specs.append(piece)
        args.append(recv)
    return pl.pallas_call(
        body,
        out_shape=[jax.ShapeDtypeStruct((2, 512, 1024), F32), TOKEN],
        grid_spec=pltpu.PrefetchScalarGridSpec(
            num_scalar_prefetch=1, grid=(steps,), in_specs=in_specs + [ANY], out_specs=[piece, TOKEN_SPEC],
            scratch_shapes=[pltpu.VMEM((512, 1024), F32), pltpu.VMEM((1024, 512), F32)],
        ),
        compiler_params=PARAMS,
    )(scal, *args, dep)


def pack_call(layer, start, count, scal, u_all, dep, weights=()):
    nw = len(weights)

    def body(*refs):
        ins, outs = refs[1:2 + nw], refs[3 + nw:4 + 2 * nw]
        for a, b in zip(ins, outs):
            b[...] = a[...]
        refs[-1][...] = jnp.zeros((8, 128), F32)

    w_in = pl.BlockSpec((None, 512, 1024), lambda e, i, s: (layer, i, 0))
    w_out = pl.BlockSpec((None, 512, 1024), lambda e, i, s: (0, i, 0))
    return pl.pallas_call(
        body,
        out_shape=[jax.ShapeDtypeStruct((count, T, Q), BF16)] + [jax.ShapeDtypeStruct((1, 1024, 1024), BF16)] * nw + [TOKEN],
        grid_spec=pltpu.PrefetchScalarGridSpec(
            num_scalar_prefetch=1, grid=(count, 2),
            in_specs=[pl.BlockSpec((None, None, 512, Q), lambda e, i, s: (layer, (1 - s[0]) * E + start + e, i, 0))] + [w_in] * nw + [ANY],
            out_specs=[pl.BlockSpec((None, 512, Q), lambda e, i, s: (e, i, 0))] + [w_out] * nw + [TOKEN_SPEC],
        ),
        compiler_params=PARAMS,
    )(scal, u_all, *weights, dep)


def final_call(layer, num_layers, total, keep, y_recv, noise_up, noise_down, clip_up, clip_down, noise_mult, outs, dep):
    def body(*refs):
        k1, k2, y1, y2, n1, n2, cu, cd, sg = refs[:9]
        up, down, tok_ref = refs[-3:]
        up[...] = (k1[...] + y1[...] + (sg[0] * cu[layer]) * n1[...]) / total
        down[...] = (k2[...] + y2[...] + (sg[0] * cd[layer]) * n2[...]) / total
        tok_ref[...] = jnp.zeros((8, 128), F32)

    s1 = pl.BlockSpec((None, 512, 512), lambda j: (0, 0, j))
    s2 = pl.BlockSpec((None, 512, 512), lambda j: (1, 0, j))
    up_spec = pl.BlockSpec((None, 512, 512), lambda j: (layer, 0, j))
    down_spec = pl.BlockSpec((None, 512, 512), lambda j: (layer, j, 0))
    in_specs = [s1, s2, s1, s2, up_spec, down_spec, SMEM, SMEM, SMEM, ANY]
    args = [keep, keep, y_recv, y_recv, noise_up, noise_down, clip_up, clip_down, noise_mult, dep]
    aliases = {}
    if outs is not None:
        in_specs += [ANY, ANY]
        args += list(outs)
        aliases = {10: 0, 11: 1}
    up, down, tok = pl.pallas_call(
        body,
        out_shape=[jax.ShapeDtypeStruct((num_layers, 512, 1024), F32), jax.ShapeDtypeStruct((num_layers, 1024, 512), F32), TOKEN],
        grid=(2,),
        in_specs=in_specs,
        out_specs=[up_spec, down_spec, TOKEN_SPEC],
        input_output_aliases=aliases,
        compiler_params=PARAMS,
    )(*args)
    return (up, down), tok


def program_order(num_layers):
    top = num_layers - 1
    order = [("k", "pack", top, 0), ("p", "u", top, 0), ("p", "w", top, 0), ("p", "w", top, 1)]
    order += [("k", "pack", top, 1), ("p", "u", top, 1), ("p", "w", 0, 0), ("p", "w", 0, 1)]

    def chain(layer, e):
        steps = [("k", "chain", layer, e)]
        if e == E - 1:
            steps.append(("p", "n", layer, 0))
        if layer > 0 and e != E - 2:
            steps += [("p", "x", layer, k) for k in ((E - 2, E - 1) if e == E - 1 else (e,))]
        if layer == top and e == 0:
            steps.append(("k", "norm", layer, e))
        if layer > 0 and e == 1:
            steps.append(("p", "u", layer - 1, E))
        return steps

    def give(layer):
        return [("k", "wgrad", layer, 1), ("p", "c", layer, 0)]

    def own(layer):
        return [("k", "wgrad", layer, 0), ("p", "y", layer, 0)]

    for layer in range(top, 0, -1):
        order += chain(layer, 0) + chain(layer, 1) + chain(layer, 2)
        if layer < top:
            order += give(layer + 1)
        order += chain(layer, 3)
        if layer + 2 <= top:
            order.append(("k", "final", layer + 2, 0))
        if layer < top:
            order += own(layer + 1)
    order += chain(0, 0) + give(1) + chain(0, 1) + own(1) + chain(0, 2) + chain(0, 3) + [("k", "final", 2, 0)]
    order += [("k", "piece1", 0, 0), ("p", "c", 0, 0), ("k", "piece1", 0, 1), ("p", "c", 0, 1)]
    order += [("k", "piece0", 0, 0), ("p", "y", 0, 0), ("k", "piece0", 0, 1), ("k", "final", 1, 0), ("k", "final", 0, 0)]
    return order


def solution(mesh):
    in_specs = (P(None, "dp", None, None), P(None, "dp", None, "tp"), P(None, None, "tp"), P(None, "tp", None), P("dp", None, None), P(None, "dp", "tp"), P(None, "tp", "dp"), P(), P(), P())
    out_specs = (P(None, "dp", "tp"), P(None, "tp", "dp"))
    swap_core = [(0, 1), (1, 0), (2, 3), (3, 2)]
    swap_x = [(0, 2), (2, 0), (1, 3), (3, 1)]
    swap_dp = [(0, 1), (1, 0)]
    num_layers = 6

    def local_step(x_stored, u_stored, w_up, w_down, d_out, noise_up, noise_down, clip_up, clip_down, noise_mult):
        total = float(d_out.shape[0] * mesh.shape["dp"])
        top = num_layers - 1
        scal = jnp.stack([lax.axis_index("tp") % 2, lax.axis_index("dp")]).astype(jnp.int32)
        tok = jnp.zeros((8, 128), F32)
        bufs, norms, part, part_recv, packed, u_recv, w_pack, w_recv = {}, {}, {}, {}, {}, {}, {}, {}
        pieces = {}
        norms_recv, give, recv, y_send, keep, y_recv = {}, {}, {}, {}, {}, {}
        outs = None
        for step in program_order(num_layers):
            kind, what, layer, k = step
            first, last = layer == top, layer == 0
            if kind == "p":
                if what == "u":
                    u_recv[layer, k] = lax.ppermute(packed[layer, k], "tp", swap_core)
                elif what == "w":
                    w_recv[layer, k] = lax.ppermute(w_pack[k] if first else (w_down, w_up)[k], "tp", swap_core)
                elif what == "n":
                    norms_recv[layer] = lax.ppermute(norms[layer], "tp", swap_x)
                elif what == "x":
                    part_recv[layer, k] = lax.ppermute(part[layer, k], "tp", swap_x)
                elif what == "c":
                    if last:
                        pieces[2, k] = lax.ppermute(pieces[1, k], "tp", swap_core)
                    else:
                        recv[layer] = lax.ppermute(give[layer], "tp", swap_core)
                else:
                    y_recv[layer] = lax.ppermute(y_send[layer], "dp", swap_dp)
            elif what == "pack":
                if first and k == 0:
                    packed[layer, k], w_pack[0], w_pack[1], tok = pack_call(layer, 0, 1, scal, u_stored, tok, (w_down, w_up))
                else:
                    packed[layer, k], tok = pack_call(layer, 1, E - 1, scal, u_stored, tok)
            elif what == "chain":
                w_at = top if first else 0
                bufs[layer], norms[layer], part[layer, k], packed[layer - 1, E], tok = chain_call(
                    layer, k, first, last, not (first and k == 0), scal,
                    d_out if first else bufs[layer + 1][0], None if first else part[layer + 1, k], None if first else part_recv[layer + 1, k],
                    u_stored, u_recv[layer, min(k, 1) if first else E], x_stored,
                    w_down, w_recv[w_at, 0], w_up, w_recv[w_at, 1], bufs.get(layer), norms.get(layer), packed.get((layer - 1, E)), tok,
                )
            elif what == "norm":
                norms[layer], tok = norm_call(layer, k, scal, x_stored, bufs[layer], tok)
            elif what == "wgrad":
                got = weight_call(
                    layer, k, x_stored, bufs[layer], norms[layer], norms_recv[layer], clip_up, clip_down, scal, recv.get(layer), tok
                )
                tok = got[-1]
                if k == 1:
                    give[layer] = got[0]
                else:
                    y_send[layer], keep[layer] = got[:2]
            elif what in ("piece1", "piece0"):
                half = int(what[-1])
                pieces[half, k], tok = weight_piece_call(
                    layer, half, k, x_stored, bufs[layer], norms[layer], norms_recv[layer], clip_up, clip_down, scal, pieces.get((2, k)), tok
                )
                if half == 0:
                    (y_send, keep)[k][layer] = pieces[0, k]
            else:
                outs, tok = final_call(
                    layer, num_layers, total, keep[layer], y_recv[layer], noise_up, noise_down, clip_up, clip_down, noise_mult, outs, tok
                )
        return outs

    return jax.shard_map(local_step, mesh=mesh, in_specs=in_specs, out_specs=out_specs, check_vma=False)
```

```python
import math
import jax
import jax.numpy as jnp
from jax import lax
from jax.experimental import pallas as pl
from jax.experimental.pallas import tpu as pltpu
from jax.sharding import PartitionSpec as P


GELU_SCALE = math.sqrt(2.0 / math.pi)

T = 1024
D = 1024
Q = 1024
E = 4
TB = 512
NB = T // TB
GB = 256
F32 = jnp.float32
BF16 = jnp.bfloat16
ANY = pl.BlockSpec(memory_space=pl.ANY)
SMEM = pl.BlockSpec(memory_space=pltpu.SMEM)
TOKEN = jax.ShapeDtypeStruct((8, 128), F32)
TOKEN_SPEC = pl.BlockSpec((8, 128), lambda *_: (0, 0))
NT = (((1,), (1,)), ((), ()))
TN = (((0,), (0,)), ((), ()))
CHAIN_FORM = ((False, True, 512), (True, True, 512), (True, False, 256), (True, False, 512), (False, True, 512), (False, True, 512))
WGRAD_FORM = ((512, True), (1024, True), (512, False), (1024, False), (512, False), (1024, True))
PARAMS = pltpu.CompilerParams(vmem_limit_bytes=63 * 1024 * 1024)


def gelu_pair(u):
    u2 = u * u
    t = jnp.tanh(u * (GELU_SCALE + (GELU_SCALE * 0.044715) * u2))
    half = 0.5 + 0.5 * t
    slope = half + (u * (1.0 - t * t)) * (0.5 * GELU_SCALE + (0.5 * GELU_SCALE * 0.134145) * u2)
    return u * half, slope


def block(i, size):
    return pl.ds(pl.multiple_of(i * size, size), size)


def gram(ref, rows, cols):
    return lax.dot_general(ref[rows, :], ref[cols, :], NT, preferred_element_type=F32)


def fold(p):
    return jnp.sum(p.reshape(p.shape[0] // 8, 8, GB), axis=0)


def ring_rows(k):
    return slice(0, 2 * GB) if k == 3 else slice(k * GB, (k + 2) * GB)


SINGLES = ((3, 3, 1.0), (2, 0, 2.0))


def single_block(r, c):
    return slice(r * GB, (r + 1) * GB), slice(c * GB, (c + 1) * GB)


def gram_x_ring(k, x_ref, ring_ref):
    ring_ref[k] = gram(x_ref, ring_rows(k), slice(k * GB, (k + 1) * GB))


def gram_x_single(k, x_ref, single_ref):
    single_ref[k] = gram(x_ref, *single_block(*SINGLES[k][:2]))


def gram_norms(ring_ref, single_ref, dz_ref, dh_ref, h_ref):
    def ring(k, sums):
        at = jnp.where(k == 3, 0, k)
        w = jnp.where(k == 3, 2.0, 1.0)
        rows, cols = pl.ds(pl.multiple_of(at * GB, GB), 2 * GB), block(k, GB)
        p1 = ring_ref[k] * gram(dh_ref, rows, cols)
        p2 = gram(h_ref, rows, cols) * gram(dz_ref, rows, cols)
        return tuple(t + (w * fold(p[:GB]) + 2.0 * fold(p[GB:])) for t, p in zip(sums, (p1, p2)))

    n1, n2 = lax.fori_loop(0, 4, ring, (jnp.zeros((8, GB), F32), jnp.zeros((8, GB), F32)))
    for k, (r, c, w) in enumerate(SINGLES):
        rows, cols = single_block(r, c)
        n1 = n1 + w * fold(single_ref[k] * gram(dh_ref, rows, cols))
        n2 = n2 + w * fold(gram(h_ref, rows, cols) * gram(dz_ref, rows, cols))
    return jnp.sum(n1), jnp.sum(n2)


GRAM_SCRATCH = (pltpu.VMEM((4, 2 * GB, GB), F32), pltpu.VMEM((2, GB, GB), F32))


def store_norms(n_ref, tok_ref, n1, n2):
    n_ref[0] = jnp.full((8, 128), n1, F32)
    n_ref[1] = jnp.full((8, 128), n2, F32)
    tok_ref[...] = jnp.zeros((8, 128), F32)


NORM_SHAPE = jax.ShapeDtypeStruct((E, 2, 8, 128), F32)


def norm_spec(ex):
    return pl.BlockSpec((None, 2, 8, 128), lambda *_: (ex, 0, 0, 0))


def chain_call(layer, ex, first, last, norms, scal, dz_prev, part_own, part_recv, u_all, u_recv, x_all, w_down, w_down_r, w_up, w_up_r, bufs, norm_buf, pack_buf, dep):
    packs = not last and ex < 2
    at_u = ex if u_recv.shape[0] == E else (ex - 1 if u_recv.shape[0] > 1 else 0)
    at_w = layer if w_down_r.shape[0] > 1 else 0
    names = ["scal", "dz"]
    args = [scal, dz_prev]
    if not first:
        names += ["po", "pr"]
        args += [part_own, part_recv]
    names += ["uo", "ur", "w2o", "w2r"]
    args += [u_all, u_recv, w_down, w_down_r]
    if norms:
        names.append("x")
        args.append(x_all)
    if not last:
        names += ["w1o", "w1r"]
        args += [w_up, w_up_r]
    names.append("dep")
    args.append(dep)
    out_names = ["dz_out", "dh_out", "h_out", "tok"]
    out_shape = [jax.ShapeDtypeStruct((E, T, D), BF16), jax.ShapeDtypeStruct((E, T, 2 * Q), BF16), jax.ShapeDtypeStruct((E, T, 2 * Q), BF16), TOKEN]
    out_specs = [ANY, ANY, ANY, TOKEN_SPEC]
    aliases = {}
    if bufs is not None:
        for k, b in enumerate(bufs):
            aliases[len(args)] = k
            names.append(f"b{k}")
            args.append(b)
    if norms:
        if norm_buf is not None:
            aliases[len(args)] = len(out_names)
            names.append("bn")
            args.append(norm_buf)
        out_names.append("n_out")
        out_shape.append(NORM_SHAPE)
        out_specs.append(norm_spec(ex))
    if not last:
        out_names.append("part_out")
        out_shape.append(jax.ShapeDtypeStruct((T, D), BF16))
        out_specs.append(ANY)
    if packs:
        if pack_buf is not None:
            aliases[len(args)] = len(out_names)
            names.append("bp")
            args.append(pack_buf)
        out_names.append("pack_out")
        out_shape.append(jax.ShapeDtypeStruct((E, T, Q), BF16))
        out_specs.append(ANY)
    scratch = {
        "dzp": pltpu.VMEM((T, D), BF16), "po_s": pltpu.VMEM((T, D), BF16), "pr_s": pltpu.VMEM((T, D), BF16),
        "u_s": pltpu.VMEM((2, T, Q), BF16), "x_s": pltpu.VMEM((T, D), BF16), "w2_s": pltpu.VMEM((2 * Q, D), BF16), "w1_s": pltpu.VMEM((2, D, Q), BF16),
        "dz_s": pltpu.VMEM((T, D), BF16), "dh_s": pltpu.VMEM((T, 2 * Q), BF16), "h_s": pltpu.VMEM((T, 2 * Q), BF16), "part_s": pltpu.VMEM((T, D), BF16),
        "ring_s": GRAM_SCRATCH[0], "single_s": GRAM_SCRATCH[1],
        "in_sem": pltpu.SemaphoreType.DMA((NB, 5)), "w_sem": pltpu.SemaphoreType.DMA((7,)), "out_sem": pltpu.SemaphoreType.DMA((NB, 4)),
        "pk_s": pltpu.VMEM((2, T, Q), BF16), "pk_sem": pltpu.SemaphoreType.DMA((2, 2)),
    }

    def body(*refs):
        r = dict(zip(names + out_names + list(scratch), refs))
        here = r["scal"][0] * E + ex
        in_sem, w_sem, out_sem = r["in_sem"], r["w_sem"], r["out_sem"]
        dz_src = r["dz"].at[here] if first else r["dz"].at[ex]

        def inputs(i):
            rows = block(i, TB)
            copies = [pltpu.make_async_copy(dz_src.at[rows], r["dzp"].at[rows], in_sem.at[i, 0])]
            if not first:
                copies += [
                    pltpu.make_async_copy(r["po"].at[rows], r["po_s"].at[rows], in_sem.at[i, 1]),
                    pltpu.make_async_copy(r["pr"].at[rows], r["pr_s"].at[rows], in_sem.at[i, 2]),
                ]
            copies += [
                pltpu.make_async_copy(r["uo"].at[layer, here, rows], r["u_s"].at[0, rows], in_sem.at[i, 3]),
                pltpu.make_async_copy(r["ur"].at[at_u, rows], r["u_s"].at[1, rows], in_sem.at[i, 4]),
            ]
            return copies

        def outputs(i):
            rows = block(i, TB)
            return [
                pltpu.make_async_copy(r["dz_s"].at[rows], r["dz_out"].at[ex, rows], out_sem.at[i, 0]),
                pltpu.make_async_copy(r["dh_s"].at[rows], r["dh_out"].at[ex, rows], out_sem.at[i, 1]),
                pltpu.make_async_copy(r["h_s"].at[rows], r["h_out"].at[ex, rows], out_sem.at[i, 2]),
            ]

        def part_output(i):
            rows = block(i, TB)
            return pltpu.make_async_copy(r["part_s"].at[rows], r["part_out"].at[rows], out_sem.at[i, 3])

        w2 = [
            pltpu.make_async_copy(
                (r["w2o"].at[layer] if c < 2 else r["w2r"].at[at_w]).at[pl.ds((c % 2) * 512, 512)], r["w2_s"].at[pl.ds(c * 512, 512)], w_sem.at[c]
            )
            for c in range(4)
        ]
        ins = [inputs(i) for i in range(NB)]
        flat, late, wide = CHAIN_FORM[layer]
        now = ins[0][:-2] + [w2[0], ins[0][-2], w2[1], w2[2], ins[0][-1], w2[3]]
        later = []
        if norms:
            x_copy = pltpu.make_async_copy(r["x"].at[layer, here], r["x_s"], w_sem.at[4])
            (now if flat else later).append(x_copy)
        later = ins[1] + later
        if not last:
            w1 = [
                pltpu.make_async_copy(r["w1o"].at[layer], r["w1_s"].at[0], w_sem.at[5]),
                pltpu.make_async_copy(r["w1r"].at[at_w], r["w1_s"].at[1], w_sem.at[6]),
            ]
            later = w1 + later
        if packs:
            there = (1 - r["scal"][0]) * E
            pack_in = [pltpu.make_async_copy(r["uo"].at[layer - 1, there + 2 * ex + j], r["pk_s"].at[j], r["pk_sem"].at[0, j]) for j in range(2)]
            pack_out = [pltpu.make_async_copy(r["pk_s"].at[j], r["pack_out"].at[2 * ex + j], r["pk_sem"].at[1, j]) for j in range(2)]
            later += pack_in
        for c in now + ([] if late else later):
            c.start()

        def store_dz(rows):
            if first:
                r["dz_s"][rows, :] = r["dzp"][rows, :]
            else:
                r["dz_s"][rows, :] = (r["dzp"][rows, :].astype(F32) + (r["po_s"][rows, :].astype(F32) + r["pr_s"][rows, :].astype(F32))).astype(BF16)

        def back_chunk(rows, c):
            for lo in range(c * 512, (c + 1) * 512, wide):
                cols, part = slice(lo, lo + wide), slice(lo % Q, lo % Q + wide)
                back = lax.dot_general(r["dz_s"][rows, :], r["w2_s"][cols, :], NT, preferred_element_type=F32)
                val, slope = gelu_pair(r["u_s"][c // 2, rows, part].astype(F32))
                r["dh_s"][rows, cols] = (slope * back).astype(BF16)
                r["h_s"][rows, cols] = val.astype(BF16)

        def part_chunk(rows, c):
            cols = slice(c * 512, (c + 1) * 512)
            acc = lax.dot_general(r["dh_s"][rows, :Q], r["w1_s"][0, cols, :], NT, preferred_element_type=F32)
            acc = acc + lax.dot_general(r["dh_s"][rows, Q:], r["w1_s"][1, cols, :], NT, preferred_element_type=F32)
            r["part_s"][rows, cols] = acc.astype(BF16)

        rows0, rows1 = slice(0, TB), slice(TB, T)
        if flat:
            for o in ins[0][:-2]:
                o.wait()
            store_dz(rows0)
            for o in now[-(len(now) - len(ins[0][:-2])):]:
                o.wait()
            if late:
                for o in later:
                    o.start()
            for c in range(4):
                back_chunk(rows0, c)
                if norms:
                    gram_x_ring(c, r["x_s"], r["ring_s"])
            for o in ins[1][:-2]:
                o.wait()
            store_dz(rows1)
            for o in ins[1][-2:] + ([] if last else w1):
                o.wait()
            for c in range(4):
                back_chunk(rows1, c)
                if c == 0:
                    for o in outputs(0):
                        o.start()
                if norms and c < 2:
                    gram_x_single(c, r["x_s"], r["single_s"])
                if not last and c % 2 == 1:
                    part_chunk(rows0, c // 2)
            if packs:
                for p, q in zip(pack_in, pack_out):
                    p.wait()
                    q.start()
            if not last:
                part_chunk(rows1, 0)
                part_output(0).start()
                part_chunk(rows1, 1)
                part_output(1).start()
            for o in outputs(1):
                o.start()
        else:
            for o in now[len(ins[0][:-2]):]:
                o.wait()
            for o in ins[0][:-2]:
                o.wait()
            if late:
                for o in later:
                    o.start()

            def rows_step(i, carry):
                rows = block(i, TB)

                @pl.when(i > 0)
                def _():
                    for o in ins[1]:
                        o.wait()

                store_dz(rows)
                for c in range(4):
                    back_chunk(rows, c)
                if not last:

                    @pl.when(i == 0)
                    def _():
                        for o in w1:
                            o.wait()

                    part_chunk(rows, 0)
                    part_chunk(rows, 1)
                for o in outputs(i):
                    o.start()
                if not last:
                    part_output(i).start()
                return carry

            lax.fori_loop(0, NB, rows_step, 0)
            if packs:
                for p, q in zip(pack_in, pack_out):
                    p.wait()
                    q.start()
            if norms:
                x_copy.wait()
                for k in range(4):
                    gram_x_ring(k, r["x_s"], r["ring_s"])
                for k in range(2):
                    gram_x_single(k, r["x_s"], r["single_s"])
        if norms:
            store_norms(r["n_out"], r["tok"], *gram_norms(r["ring_s"], r["single_s"], r["dz_s"], r["dh_s"], r["h_s"]))
        else:
            r["tok"][...] = jnp.zeros((8, 128), F32)
        for i in range(NB):
            for c in outputs(i):
                c.wait()
            if not last:
                part_output(i).wait()
        if packs:
            for b in pack_out:
                b.wait()

    outs = pl.pallas_call(
        body,
        out_shape=out_shape,
        in_specs=[SMEM] + [ANY] * (len(args) - 1),
        out_specs=out_specs,
        scratch_shapes=list(scratch.values()),
        input_output_aliases=aliases,
        compiler_params=PARAMS,
        grid=(1,),
    )(*args)
    named = dict(zip(out_names, outs))
    return outs[:3], named.get("n_out", norm_buf), named.get("part_out"), named.get("pack_out", pack_buf), named["tok"]


def norm_call(layer, ex, scal, x_all, bufs, dep):
    def body(s_ref, x_ref, dz_ref, dh_ref, h_ref, dep_ref, n_ref, tok_ref, ring_ref, single_ref):
        for k in range(4):
            gram_x_ring(k, x_ref, ring_ref)
        for k in range(2):
            gram_x_single(k, x_ref, single_ref)
        store_norms(n_ref, tok_ref, *gram_norms(ring_ref, single_ref, dz_ref, dh_ref, h_ref))

    def at(width):
        return pl.BlockSpec((None, T, width), lambda i, s: (ex, 0, 0))

    return pl.pallas_call(
        body,
        out_shape=[NORM_SHAPE, TOKEN],
        grid_spec=pltpu.PrefetchScalarGridSpec(
            num_scalar_prefetch=1, grid=(1,),
            in_specs=[pl.BlockSpec((None, None, T, D), lambda i, s: (layer, s[0] * E + ex, 0, 0)), at(D), at(2 * Q), at(2 * Q), ANY],
            out_specs=[norm_spec(ex), TOKEN_SPEC], scratch_shapes=GRAM_SCRATCH,
        ),
        compiler_params=PARAMS,
    )(scal, x_all, *bufs, dep)


def weight_call(layer, half, x_all, bufs, norms, norms_recv, clip_up, clip_down, scal, recv, dep):
    dz, dh, hid = bufs
    own = half == 0
    kb, split = WGRAD_FORM[layer]
    steps = E * T // kb
    per = T // kb

    def body(*refs):
        refs = list(refs)
        s_ref, x_ref, dh_ref, h_ref, dz_ref, no_ref, nr_ref, cu_ref, cd_ref = refs[:9]
        del refs[:9]
        if own:
            recv_ref = refs.pop(0)
        refs.pop(0)
        if own:
            send_ref, keep_ref, tok_ref, acc, recv_s, sem, recv_sem = refs
        else:
            g_ref, tok_ref, acc, sem = refs
        k = pl.program_id(0)
        n = no_ref[...] + nr_ref[...]
        c1 = jnp.minimum(1.0, cu_ref[layer] / jnp.sqrt(n[0, 0:1, 0:1]))
        c2 = jnp.minimum(1.0, cd_ref[layer] / jnp.sqrt(n[1, 0:1, 0:1]))
        y = s_ref[1]
        halves = (1 - y, y) if own else (0, 1)
        if own:
            recv_copy = pltpu.make_async_copy(recv_ref, recv_s, recv_sem)

        def copies(g, at):
            ds = block(halves[at], 512)
            if not own:
                part = (0, ds) if g == 0 else (1, slice(None), ds)
                return [pltpu.make_async_copy(acc.at[part], g_ref.at[part], sem.at[g, at, 0])]
            out = (send_ref, keep_ref)[at]
            if g == 0:
                return [pltpu.make_async_copy(acc.at[0, ds], out.at[0], sem.at[g, at, 0])]
            return [
                pltpu.make_async_copy(acc.at[1, pl.ds(b * 512, 512), ds], out.at[1, :, pl.ds(b * 512, 512)], sem.at[g, at, b])
                for b in range(2)
            ]

        @pl.when(k == 0)
        def _():
            tok_ref[...] = jnp.zeros((8, 128), F32)
            if own:
                recv_copy.start()

        def add(init, final):
            dhc = (dh_ref[...].astype(F32) * c1).astype(BF16)
            if final and own:
                recv_copy.wait()
            if split:
                started = []
                for at in range(2):
                    ds = block(halves[at], 512)
                    for g in range(2):
                        if g == 0:
                            part = (0, ds)
                            new = lax.dot_general(x_ref[:, ds], dhc, TN, preferred_element_type=F32)
                        else:
                            part = (1, slice(None), ds)
                            new = lax.dot_general(h_ref[...], (dz_ref[:, ds].astype(F32) * c2).astype(BF16), TN, preferred_element_type=F32)
                        if not init:
                            new = acc[part] + new
                        if final and own:
                            new = new + recv_s[part]
                        acc[part] = new
                        if final:
                            if started:
                                for c in copies(*started[-1]):
                                    c.start()
                            started.append((g, at))
                if final:
                    for c in copies(*started[-1]):
                        c.start()
                    for s in started:
                        for c in copies(*s):
                            c.wait()
            else:
                for g in range(2):
                    if g == 0:
                        new = lax.dot_general(x_ref[...], dhc, TN, preferred_element_type=F32)
                    else:
                        new = lax.dot_general(h_ref[...], (dz_ref[...].astype(F32) * c2).astype(BF16), TN, preferred_element_type=F32)
                    if not init:
                        new = acc[g] + new
                    if final and own:
                        new = new + recv_s[g]
                    acc[g] = new
                if final:
                    sent = [c for at in range(2) for g in range(2) for c in copies(g, at)]
                    for c in sent:
                        c.start()
                    for c in sent:
                        c.wait()

        @pl.when(k == 0)
        def _():
            add(True, False)

        @pl.when((k > 0) & (k < steps - 1))
        def _():
            add(False, False)

        @pl.when(k == steps - 1)
        def _():
            add(False, True)

    norm_in = pl.BlockSpec((None, 2, 8, 128), lambda k, s: (k // per, 0, 0, 0))
    in_specs = [
        pl.BlockSpec((None, None, kb, D), lambda k, s: (layer, s[0] * E + k // per, k % per, 0)),
        pl.BlockSpec((None, kb, Q), lambda k, s: (k // per, k % per, half)),
        pl.BlockSpec((None, kb, Q), lambda k, s: (k // per, k % per, half)),
        pl.BlockSpec((None, kb, D), lambda k, s: (k // per, k % per, 0)),
        norm_in, norm_in, SMEM, SMEM,
    ]
    args = [x_all, dh, hid, dz, norms, norms_recv, clip_up, clip_down]
    piece = jax.ShapeDtypeStruct((2, 512, 1024), F32)
    scratch = [pltpu.VMEM((2, 1024, 1024), F32)]
    if own:
        in_specs.append(ANY)
        args.append(recv)
        out_shape, out_specs = [piece, piece, TOKEN], [ANY, ANY, TOKEN_SPEC]
        scratch += [pltpu.VMEM((2, 1024, 1024), F32), pltpu.SemaphoreType.DMA((2, 2, 2)), pltpu.SemaphoreType.DMA]
    else:
        out_shape, out_specs = [jax.ShapeDtypeStruct((2, 1024, 1024), F32), TOKEN], [ANY, TOKEN_SPEC]
        scratch += [pltpu.SemaphoreType.DMA((2, 2, 2))]
    return pl.pallas_call(
        body,
        out_shape=out_shape,
        grid_spec=pltpu.PrefetchScalarGridSpec(
            num_scalar_prefetch=1, grid=(steps,), in_specs=in_specs + [ANY], out_specs=out_specs, scratch_shapes=scratch,
        ),
        compiler_params=PARAMS,
    )(scal, *args, dep)


def weight_piece_call(layer, half, at, x_all, bufs, norms, norms_recv, clip_up, clip_down, scal, recv, dep):
    dz, dh, hid = bufs
    own = half == 0
    steps = E

    def body(*refs):
        refs = list(refs)
        _, x_ref, dh_ref, h_ref, dz_ref, no_ref, nr_ref, cu_ref, cd_ref = refs[:9]
        del refs[:9]
        if own:
            recv_ref = refs.pop(0)
        refs.pop(0)
        out_ref, tok_ref, acc1, acc2 = refs
        k = pl.program_id(0)
        n = no_ref[...] + nr_ref[...]
        c1 = jnp.minimum(1.0, cu_ref[layer] / jnp.sqrt(n[0, 0:1, 0:1]))
        c2 = jnp.minimum(1.0, cd_ref[layer] / jnp.sqrt(n[1, 0:1, 0:1]))

        def products():
            g1 = lax.dot_general(x_ref[...], (dh_ref[...].astype(F32) * c1).astype(BF16), TN, preferred_element_type=F32)
            g2 = lax.dot_general(h_ref[...], (dz_ref[...].astype(F32) * c2).astype(BF16), TN, preferred_element_type=F32)
            return g1, g2

        @pl.when(k == 0)
        def _():
            tok_ref[...] = jnp.zeros((8, 128), F32)
            acc1[...], acc2[...] = products()

        @pl.when((k > 0) & (k < steps - 1))
        def _():
            g1, g2 = products()
            acc1[...] += g1
            acc2[...] += g2

        @pl.when(k == steps - 1)
        def _():
            g1, g2 = products()
            g1 = acc1[...] + g1
            g2 = acc2[...] + g2
            if own:
                g1 = g1 + recv_ref[0]
            out_ref[0] = g1
            for b in range(2):
                cols = slice(b * 512, (b + 1) * 512)
                out_ref[1, :, cols] = g2[cols] + recv_ref[1, :, cols] if own else g2[cols]

    def d_half(s):
        return 1 - s[1] if at == 0 else s[1]

    norm_in = pl.BlockSpec((None, 2, 8, 128), lambda k, s: (k, 0, 0, 0))
    piece = pl.BlockSpec((2, 512, 1024), lambda k, s: (0, 0, 0))
    in_specs = [
        pl.BlockSpec((None, None, T, 512), lambda k, s: (layer, s[0] * E + k, 0, d_half(s))),
        pl.BlockSpec((None, T, Q), lambda k, s: (k, 0, half)),
        pl.BlockSpec((None, T, Q), lambda k, s: (k, 0, half)),
        pl.BlockSpec((None, T, 512), lambda k, s: (k, 0, d_half(s))),
        norm_in, norm_in, SMEM, SMEM,
    ]
    args = [x_all, dh, hid, dz, norms, norms_recv, clip_up, clip_down]
    if own:
        in_specs.append(piece)
        args.append(recv)
    return pl.pallas_call(
        body,
        out_shape=[jax.ShapeDtypeStruct((2, 512, 1024), F32), TOKEN],
        grid_spec=pltpu.PrefetchScalarGridSpec(
            num_scalar_prefetch=1, grid=(steps,), in_specs=in_specs + [ANY], out_specs=[piece, TOKEN_SPEC],
            scratch_shapes=[pltpu.VMEM((512, 1024), F32), pltpu.VMEM((1024, 512), F32)],
        ),
        compiler_params=PARAMS,
    )(scal, *args, dep)


def pack_call(layer, start, count, scal, u_all, dep, weights=()):
    nw = len(weights)

    def body(*refs):
        ins, outs = refs[1:2 + nw], refs[3 + nw:4 + 2 * nw]
        for a, b in zip(ins, outs):
            b[...] = a[...]
        refs[-1][...] = jnp.zeros((8, 128), F32)

    w_in = pl.BlockSpec((None, 512, 1024), lambda e, i, s: (layer, i, 0))
    w_out = pl.BlockSpec((None, 512, 1024), lambda e, i, s: (0, i, 0))
    return pl.pallas_call(
        body,
        out_shape=[jax.ShapeDtypeStruct((count, T, Q), BF16)] + [jax.ShapeDtypeStruct((1, 1024, 1024), BF16)] * nw + [TOKEN],
        grid_spec=pltpu.PrefetchScalarGridSpec(
            num_scalar_prefetch=1, grid=(count, 2),
            in_specs=[pl.BlockSpec((None, None, 512, Q), lambda e, i, s: (layer, (1 - s[0]) * E + start + e, i, 0))] + [w_in] * nw + [ANY],
            out_specs=[pl.BlockSpec((None, 512, Q), lambda e, i, s: (e, i, 0))] + [w_out] * nw + [TOKEN_SPEC],
        ),
        compiler_params=PARAMS,
    )(scal, u_all, *weights, dep)


def final_call(layer, num_layers, total, keep, y_recv, noise_up, noise_down, clip_up, clip_down, noise_mult, outs, dep):
    def body(*refs):
        k1, k2, y1, y2, n1, n2, cu, cd, sg = refs[:9]
        up, down, tok_ref = refs[-3:]
        up[...] = (k1[...] + y1[...] + (sg[0] * cu[layer]) * n1[...]) / total
        down[...] = (k2[...] + y2[...] + (sg[0] * cd[layer]) * n2[...]) / total
        tok_ref[...] = jnp.zeros((8, 128), F32)

    s1 = pl.BlockSpec((None, 512, 512), lambda j: (0, 0, j))
    s2 = pl.BlockSpec((None, 512, 512), lambda j: (1, 0, j))
    up_spec = pl.BlockSpec((None, 512, 512), lambda j: (layer, 0, j))
    down_spec = pl.BlockSpec((None, 512, 512), lambda j: (layer, j, 0))
    in_specs = [s1, s2, s1, s2, up_spec, down_spec, SMEM, SMEM, SMEM, ANY]
    args = [keep, keep, y_recv, y_recv, noise_up, noise_down, clip_up, clip_down, noise_mult, dep]
    aliases = {}
    if outs is not None:
        in_specs += [ANY, ANY]
        args += list(outs)
        aliases = {10: 0, 11: 1}
    up, down, tok = pl.pallas_call(
        body,
        out_shape=[jax.ShapeDtypeStruct((num_layers, 512, 1024), F32), jax.ShapeDtypeStruct((num_layers, 1024, 512), F32), TOKEN],
        grid=(2,),
        in_specs=in_specs,
        out_specs=[up_spec, down_spec, TOKEN_SPEC],
        input_output_aliases=aliases,
        compiler_params=PARAMS,
    )(*args)
    return (up, down), tok


def program_order(num_layers):
    top = num_layers - 1
    order = [("k", "pack", top, 0), ("p", "u", top, 0), ("p", "w", top, 0), ("p", "w", top, 1)]
    order += [("k", "pack", top, 1), ("p", "u", top, 1), ("p", "w", 0, 0), ("p", "w", 0, 1)]

    def chain(layer, e):
        held = range(E - 3 if layer == 1 else E - 2, E)
        steps = [("k", "chain", layer, e)]
        if e == E - 1:
            steps.append(("p", "n", layer, 0))
        if layer > 0 and (e == E - 1 or e not in held):
            steps += [("p", "x", layer, k) for k in (held if e == E - 1 else (e,))]
        if layer == top and e == 0:
            steps.append(("k", "norm", layer, e))
        if layer > 0 and e == 1:
            steps.append(("p", "u", layer - 1, E))
        return steps

    def give(layer):
        return [("k", "wgrad", layer, 1), ("p", "c", layer, 0)]

    def own(layer):
        return [("k", "wgrad", layer, 0), ("p", "y", layer, 0)]

    for layer in range(top, 0, -1):
        order += chain(layer, 0) + chain(layer, 1) + chain(layer, 2)
        if layer < top:
            order += give(layer + 1)
        order += chain(layer, 3)
        if 1 < layer < top - 1:
            order.append(("k", "final", layer + 2, 0))
        if layer < top:
            order += own(layer + 1)
    order += give(1) + chain(0, 0) + own(1) + chain(0, 1) + chain(0, 2) + [("k", "final", 3, 0)] + chain(0, 3)
    order += [("k", "piece1", 0, 0), ("p", "c", 0, 0), ("k", "final", 2, 0), ("k", "piece0", 0, 0), ("p", "y", 0, 0)]
    order += [("k", "piece1", 0, 1), ("p", "c", 0, 1), ("k", "final", 1, 0), ("k", "piece0", 0, 1), ("k", "final", 0, 0)]
    return order


def solution(mesh):
    in_specs = (P(None, "dp", None, None), P(None, "dp", None, "tp"), P(None, None, "tp"), P(None, "tp", None), P("dp", None, None), P(None, "dp", "tp"), P(None, "tp", "dp"), P(), P(), P())
    out_specs = (P(None, "dp", "tp"), P(None, "tp", "dp"))
    swap_core = [(0, 1), (1, 0), (2, 3), (3, 2)]
    swap_x = [(0, 2), (2, 0), (1, 3), (3, 1)]
    swap_dp = [(0, 1), (1, 0)]
    num_layers = 6

    def local_step(x_stored, u_stored, w_up, w_down, d_out, noise_up, noise_down, clip_up, clip_down, noise_mult):
        total = float(d_out.shape[0] * mesh.shape["dp"])
        top = num_layers - 1
        scal = jnp.stack([lax.axis_index("tp") % 2, lax.axis_index("dp")]).astype(jnp.int32)
        tok = jnp.zeros((8, 128), F32)
        bufs, norms, part, part_recv, packed, u_recv, w_pack, w_recv = {}, {}, {}, {}, {}, {}, {}, {}
        pieces = {}
        norms_recv, give, recv, y_send, keep, y_recv = {}, {}, {}, {}, {}, {}
        outs = None
        for step in program_order(num_layers):
            kind, what, layer, k = step
            first, last = layer == top, layer == 0
            if kind == "p":
                if what == "u":
                    u_recv[layer, k] = lax.ppermute(packed[layer, k], "tp", swap_core)
                elif what == "w":
                    w_recv[layer, k] = lax.ppermute(w_pack[k] if first else (w_down, w_up)[k], "tp", swap_core)
                elif what == "n":
                    norms_recv[layer] = lax.ppermute(norms[layer], "tp", swap_x)
                elif what == "x":
                    part_recv[layer, k] = lax.ppermute(part[layer, k], "tp", swap_x)
                elif what == "c":
                    if last:
                        pieces[2, k] = lax.ppermute(pieces[1, k], "tp", swap_core)
                    else:
                        recv[layer] = lax.ppermute(give[layer], "tp", swap_core)
                else:
                    y_recv[layer] = lax.ppermute(y_send[layer], "dp", swap_dp)
            elif what == "pack":
                if first and k == 0:
                    packed[layer, k], w_pack[0], w_pack[1], tok = pack_call(layer, 0, 1, scal, u_stored, tok, (w_down, w_up))
                else:
                    packed[layer, k], tok = pack_call(layer, 1, E - 1, scal, u_stored, tok)
            elif what == "chain":
                w_at = top if first else 0
                bufs[layer], norms[layer], part[layer, k], packed[layer - 1, E], tok = chain_call(
                    layer, k, first, last, not (first and k == 0), scal,
                    d_out if first else bufs[layer + 1][0], None if first else part[layer + 1, k], None if first else part_recv[layer + 1, k],
                    u_stored, u_recv[layer, min(k, 1) if first else E], x_stored,
                    w_down, w_recv[w_at, 0], w_up, w_recv[w_at, 1], bufs.get(layer), norms.get(layer), packed.get((layer - 1, E)), tok,
                )
            elif what == "norm":
                norms[layer], tok = norm_call(layer, k, scal, x_stored, bufs[layer], tok)
            elif what == "wgrad":
                got = weight_call(
                    layer, k, x_stored, bufs[layer], norms[layer], norms_recv[layer], clip_up, clip_down, scal, recv.get(layer), tok
                )
                tok = got[-1]
                if k == 1:
                    give[layer] = got[0]
                else:
                    y_send[layer], keep[layer] = got[:2]
            elif what in ("piece1", "piece0"):
                half = int(what[-1])
                pieces[half, k], tok = weight_piece_call(
                    layer, half, k, x_stored, bufs[layer], norms[layer], norms_recv[layer], clip_up, clip_down, scal, pieces.get((2, k)), tok
                )
                if half == 0:
                    (y_send, keep)[k][layer] = pieces[0, k]
            else:
                outs, tok = final_call(
                    layer, num_layers, total, keep[layer], y_recv[layer], noise_up, noise_down, clip_up, clip_down, noise_mult, outs, tok
                )
        return outs

    return jax.shard_map(local_step, mesh=mesh, in_specs=in_specs, out_specs=out_specs, check_vma=False)
```

```python
import math
import jax
import jax.numpy as jnp
from jax import lax
from jax.experimental import pallas as pl
from jax.experimental.pallas import tpu as pltpu
from jax.sharding import PartitionSpec as P


GELU_SCALE = math.sqrt(2.0 / math.pi)

T = 1024
D = 1024
Q = 1024
E = 4
TB = 512
NB = T // TB
GB = 256
F32 = jnp.float32
BF16 = jnp.bfloat16
ANY = pl.BlockSpec(memory_space=pl.ANY)
SMEM = pl.BlockSpec(memory_space=pltpu.SMEM)
TOKEN = jax.ShapeDtypeStruct((8, 128), F32)
TOKEN_SPEC = pl.BlockSpec((8, 128), lambda *_: (0, 0))
NT = (((1,), (1,)), ((), ()))
TN = (((0,), (0,)), ((), ()))
PARAMS = pltpu.CompilerParams(vmem_limit_bytes=63 * 1024 * 1024)


def gelu_pair(u):
    u2 = u * u
    t = jnp.tanh(u * (GELU_SCALE + (GELU_SCALE * 0.044715) * u2))
    half = 0.5 + 0.5 * t
    slope = half + (u * (1.0 - t * t)) * (0.5 * GELU_SCALE + (0.5 * GELU_SCALE * 0.134145) * u2)
    return u * half, slope


def block(i, size):
    return pl.ds(pl.multiple_of(i * size, size), size)


def gram(ref, rows, cols):
    return lax.dot_general(ref[rows, :], ref[cols, :], NT, preferred_element_type=F32)


def fold(p):
    return jnp.sum(p.reshape(p.shape[0] // 8, 8, GB), axis=0)


def ring_rows(k):
    return slice(0, 2 * GB) if k == 3 else slice(k * GB, (k + 2) * GB)


SINGLES = ((3, 3, 1.0), (2, 0, 2.0))


def single_block(r, c):
    return slice(r * GB, (r + 1) * GB), slice(c * GB, (c + 1) * GB)


def gram_x_ring(k, x_ref, ring_ref):
    ring_ref[k] = gram(x_ref, ring_rows(k), slice(k * GB, (k + 1) * GB))


def gram_x_single(k, x_ref, single_ref):
    single_ref[k] = gram(x_ref, *single_block(*SINGLES[k][:2]))


def gram_norms(ring_ref, single_ref, dz_ref, dh_ref, h_ref):
    def ring(k, sums):
        at = jnp.where(k == 3, 0, k)
        w = jnp.where(k == 3, 2.0, 1.0)
        rows, cols = pl.ds(pl.multiple_of(at * GB, GB), 2 * GB), block(k, GB)
        p1 = ring_ref[k] * gram(dh_ref, rows, cols)
        p2 = gram(h_ref, rows, cols) * gram(dz_ref, rows, cols)
        return tuple(t + (w * fold(p[:GB]) + 2.0 * fold(p[GB:])) for t, p in zip(sums, (p1, p2)))

    n1, n2 = lax.fori_loop(0, 4, ring, (jnp.zeros((8, GB), F32), jnp.zeros((8, GB), F32)))
    for k, (r, c, w) in enumerate(SINGLES):
        rows, cols = single_block(r, c)
        n1 = n1 + w * fold(single_ref[k] * gram(dh_ref, rows, cols))
        n2 = n2 + w * fold(gram(h_ref, rows, cols) * gram(dz_ref, rows, cols))
    return jnp.sum(n1), jnp.sum(n2)


GRAM_SCRATCH = (pltpu.VMEM((4, 2 * GB, GB), F32), pltpu.VMEM((2, GB, GB), F32))


def store_norms(n_ref, tok_ref, n1, n2):
    n_ref[0] = jnp.full((8, 128), n1, F32)
    n_ref[1] = jnp.full((8, 128), n2, F32)
    tok_ref[...] = jnp.zeros((8, 128), F32)


NORM_SHAPE = jax.ShapeDtypeStruct((E, 2, 8, 128), F32)


def norm_spec(exs):
    if len(exs) == 1:
        return pl.BlockSpec((None, 2, 8, 128), lambda *_: (exs[0], 0, 0, 0))
    return pl.BlockSpec((len(exs), 2, 8, 128), lambda *_: (exs[0] // len(exs), 0, 0, 0))


def chain_call(layer, exs, blocks, first, last, norms, packs, apart, scal, dz_prev, sources, u_all, u_recv, x_all, w_down, w_down_r, w_up, w_up_r, bufs, norm_buf, pack_buf, dep):
    at_w = layer if w_down_r.shape[0] > 1 else 0
    names = ["scal", "dz"]
    args = [scal, dz_prev]
    if not first:
        for k, own, received in sorted({v[0]: v[:3] for v in sources.values()}.values(), key=lambda v: v[0]):
            names += [f"po{k}", f"pr{k}"]
            args += [own, received]
    names += ["uo", "ur", "w2o", "w2r"]
    args += [u_all, u_recv, w_down, w_down_r]
    if norms:
        names.append("x")
        args.append(x_all)
    if not last:
        names += ["w1o", "w1r"]
        args += [w_up, w_up_r]
    names.append("dep")
    args.append(dep)
    out_names = ["dz_out", "dh_out", "h_out", "tok"]
    out_shape = [jax.ShapeDtypeStruct((E, T, D), BF16), jax.ShapeDtypeStruct((E, T, 2 * Q), BF16), jax.ShapeDtypeStruct((E, T, 2 * Q), BF16), TOKEN]
    out_specs = [ANY, ANY, ANY, TOKEN_SPEC]
    aliases = {}
    if bufs is not None:
        for k, b in enumerate(bufs):
            aliases[len(args)] = k
            names.append(f"b{k}")
            args.append(b)
    if norms:
        if norm_buf is not None:
            aliases[len(args)] = len(out_names)
            names.append("bn")
            args.append(norm_buf)
        out_names.append("n_out")
        out_shape.append(NORM_SHAPE)
        out_specs.append(norm_spec(exs))
    parts = 0 if last else (len(exs) if apart else 1)
    for k in range(parts):
        out_names.append(f"part{k}")
        rows = (len(blocks) * TB, D)
        out_shape.append(jax.ShapeDtypeStruct(rows if len(exs) == 1 or apart else (len(exs), *rows), BF16))
        out_specs.append(ANY)
    if packs:
        if pack_buf is not None:
            aliases[len(args)] = len(out_names)
            names.append("bp")
            args.append(pack_buf)
        out_names.append("pack_out")
        out_shape.append(jax.ShapeDtypeStruct((E, T, Q), BF16))
        out_specs.append(ANY)
    scratch = {
        "dzp": pltpu.VMEM((T, D), BF16), "po_s": pltpu.VMEM((T, D), BF16), "pr_s": pltpu.VMEM((T, D), BF16),
        "u_s": pltpu.VMEM((2, T, Q), BF16), "x_s": pltpu.VMEM((len(exs), T, D), BF16), "w2_s": pltpu.VMEM((2 * Q, D), BF16), "w1_s": pltpu.VMEM((2, D, Q), BF16),
        "dz_s": pltpu.VMEM((T, D), BF16), "dh_s": pltpu.VMEM((T, 2 * Q), BF16), "h_s": pltpu.VMEM((T, 2 * Q), BF16), "part_s": pltpu.VMEM((T, D), BF16),
        "ring_s": GRAM_SCRATCH[0], "single_s": GRAM_SCRATCH[1],
        "in_sem": pltpu.SemaphoreType.DMA((NB, 5)), "w_sem": pltpu.SemaphoreType.DMA((4,)), "out_sem": pltpu.SemaphoreType.DMA((NB, 4)),
        "x_sem": pltpu.SemaphoreType.DMA((len(exs),)), "pk_s": pltpu.VMEM((2, T, Q), BF16), "pk_sem": pltpu.SemaphoreType.DMA((2, 2)),
    }

    def body(*refs):
        r = dict(zip(names + out_names + list(scratch), refs))
        in_sem, w_sem, out_sem = r["in_sem"], r["w_sem"], r["out_sem"]
        core0 = r["scal"][0] * E

        def inputs(ex, i):
            rows = pl.ds(i * TB, TB)
            at_u = ex if u_recv.shape[0] == E else (ex - 1 if u_recv.shape[0] > 1 else 0)
            dz_src = r["dz"].at[core0 + ex] if first else r["dz"].at[ex]
            copies = [pltpu.make_async_copy(dz_src.at[rows], r["dzp"].at[rows], in_sem.at[i, 0])]
            if not first:
                k, _, _, index = sources[ex, i]
                copies += [
                    pltpu.make_async_copy(r[f"po{k}"].at[index], r["po_s"].at[rows], in_sem.at[i, 1]),
                    pltpu.make_async_copy(r[f"pr{k}"].at[index], r["pr_s"].at[rows], in_sem.at[i, 2]),
                ]
            return copies + [
                pltpu.make_async_copy(r["uo"].at[layer, core0 + ex, rows], r["u_s"].at[0, rows], in_sem.at[i, 3]),
                pltpu.make_async_copy(r["ur"].at[at_u, rows], r["u_s"].at[1, rows], in_sem.at[i, 4]),
            ]

        def outputs(ex, i):
            rows = block(i, TB)
            copies = [
                pltpu.make_async_copy(r["dz_s"].at[rows], r["dz_out"].at[ex, rows], out_sem.at[i, 0]),
                pltpu.make_async_copy(r["dh_s"].at[rows], r["dh_out"].at[ex, rows], out_sem.at[i, 1]),
                pltpu.make_async_copy(r["h_s"].at[rows], r["h_out"].at[ex, rows], out_sem.at[i, 2]),
            ]
            if not last:
                j = exs.index(ex)
                out = r[f"part{j}"] if apart or len(exs) == 1 else r["part0"].at[j]
                copies.append(pltpu.make_async_copy(r["part_s"].at[rows], out.at[block(i - blocks[0], TB)], out_sem.at[i, 3]))
            return copies

        w2 = [
            pltpu.make_async_copy(r["w2o"].at[layer], r["w2_s"].at[pl.ds(0, Q)], w_sem.at[0]),
            pltpu.make_async_copy(r["w2r"].at[at_w], r["w2_s"].at[pl.ds(Q, Q)], w_sem.at[1]),
        ]
        w1 = []
        if not last:
            w1 = [
                pltpu.make_async_copy(r["w1o"].at[layer], r["w1_s"].at[0], w_sem.at[2]),
                pltpu.make_async_copy(r["w1r"].at[at_w], r["w1_s"].at[1], w_sem.at[3]),
            ]
        x_copies = [pltpu.make_async_copy(r["x"].at[layer, core0 + ex], r["x_s"].at[j], r["x_sem"].at[j]) for j, ex in enumerate(exs)] if norms else []
        pack_in, pack_out = [], []
        if packs:
            there = (1 - r["scal"][0]) * E
            at = 2 * exs[0]
            pack_in = [pltpu.make_async_copy(r["uo"].at[layer - 1, there + at + j], r["pk_s"].at[j], r["pk_sem"].at[0, j]) for j in range(2)]
            pack_out = [pltpu.make_async_copy(r["pk_s"].at[j], r["pack_out"].at[at + j], r["pk_sem"].at[1, j]) for j in range(2)]

        def wait_all(copies):
            for c in copies:
                c.wait()

        def start_all(copies):
            for c in copies:
                c.start()

        def back_chunk(rows, c):
            cols, part = slice(c * 512, (c + 1) * 512), slice((c % 2) * 512, (c % 2 + 1) * 512)
            back = lax.dot_general(r["dz_s"][rows, :], r["w2_s"][cols, :], NT, preferred_element_type=F32)
            val, slope = gelu_pair(r["u_s"][c // 2, rows, part].astype(F32))
            r["dh_s"][rows, cols] = (slope * back).astype(BF16)
            r["h_s"][rows, cols] = val.astype(BF16)

        def part_chunk(rows, c):
            cols = slice(c * 512, (c + 1) * 512)
            acc = lax.dot_general(r["dh_s"][rows, :Q], r["w1_s"][0, cols, :], NT, preferred_element_type=F32)
            acc = acc + lax.dot_general(r["dh_s"][rows, Q:], r["w1_s"][1, cols, :], NT, preferred_element_type=F32)
            r["part_s"][rows, cols] = acc.astype(BF16)

        start_all(inputs(exs[0], blocks[0]) + w2)
        for j, ex in enumerate(exs):
            wait_all(inputs(ex, blocks[0]) + (w2 if j == 0 else []))
            if j == 0:
                start_all(w1)
            start_all([c for i in blocks[1:] for c in inputs(ex, i)])
            if norms and j == 0:
                start_all(x_copies)
            if j == 0:
                start_all(pack_in)

            def rows_step(i, carry):
                rows = block(i, TB)
                if len(blocks) > 1:

                    @pl.when(i > blocks[0])
                    def _():
                        wait_all(inputs(ex, blocks[1]))

                if first:
                    r["dz_s"][rows, :] = r["dzp"][rows, :]
                else:
                    r["dz_s"][rows, :] = (r["dzp"][rows, :].astype(F32) + (r["po_s"][rows, :].astype(F32) + r["pr_s"][rows, :].astype(F32))).astype(BF16)
                for c in range(4):
                    back_chunk(rows, c)
                if not last:
                    if j == 0:

                        @pl.when(i == blocks[0])
                        def _():
                            wait_all(w1)

                    part_chunk(rows, 0)
                    part_chunk(rows, 1)
                start_all(outputs(ex, i))
                return carry

            lax.fori_loop(blocks[0], blocks[-1] + 1, rows_step, 0)
            if j + 1 < len(exs):
                start_all(inputs(exs[j + 1], blocks[0]))
            if j == 0:
                for p, q in zip(pack_in, pack_out):
                    p.wait()
                    q.start()
            if norms:
                x_copies[j].wait()
                for k in range(4):
                    gram_x_ring(k, r["x_s"].at[j], r["ring_s"])
                for k in range(2):
                    gram_x_single(k, r["x_s"].at[j], r["single_s"])
                n_ref = r["n_out"] if len(exs) == 1 else r["n_out"].at[j]
                store_norms(n_ref, r["tok"], *gram_norms(r["ring_s"], r["single_s"], r["dz_s"], r["dh_s"], r["h_s"]))
            else:
                r["tok"][...] = jnp.zeros((8, 128), F32)
            for i in blocks:
                wait_all(outputs(ex, i))
            if j == 0:
                wait_all(pack_out)

    outs = pl.pallas_call(
        body,
        out_shape=out_shape,
        in_specs=[SMEM] + [ANY] * (len(args) - 1),
        out_specs=out_specs,
        scratch_shapes=list(scratch.values()),
        input_output_aliases=aliases,
        compiler_params=PARAMS,
        grid=(1,),
    )(*args)
    named = dict(zip(out_names, outs))
    return outs[:3], named.get("n_out", norm_buf), [named[f"part{k}"] for k in range(parts)], named.get("pack_out", pack_buf), named["tok"]


def norm_call(layer, ex, scal, x_all, bufs, dep):
    def body(s_ref, x_ref, dz_ref, dh_ref, h_ref, dep_ref, n_ref, tok_ref, ring_ref, single_ref):
        for k in range(4):
            gram_x_ring(k, x_ref, ring_ref)
        for k in range(2):
            gram_x_single(k, x_ref, single_ref)
        store_norms(n_ref, tok_ref, *gram_norms(ring_ref, single_ref, dz_ref, dh_ref, h_ref))

    def at(width):
        return pl.BlockSpec((None, T, width), lambda i, s: (ex, 0, 0))

    return pl.pallas_call(
        body,
        out_shape=[NORM_SHAPE, TOKEN],
        grid_spec=pltpu.PrefetchScalarGridSpec(
            num_scalar_prefetch=1, grid=(1,),
            in_specs=[pl.BlockSpec((None, None, T, D), lambda i, s: (layer, s[0] * E + ex, 0, 0)), at(D), at(2 * Q), at(2 * Q), ANY],
            out_specs=[norm_spec((ex,)), TOKEN_SPEC], scratch_shapes=GRAM_SCRATCH,
        ),
        compiler_params=PARAMS,
    )(scal, x_all, *bufs, dep)


def weight_call(layer, half, x_all, bufs, norms, norms_recv, clip_up, clip_down, scal, recv, dep):
    dz, dh, hid = bufs
    own = half == 0
    steps = E

    def body(*refs):
        refs = list(refs)
        s_ref, x_ref, dh_ref, h_ref, dz_ref, no_ref, nr_ref, cu_ref, cd_ref = refs[:9]
        del refs[:9]
        if own:
            recv_ref = refs.pop(0)
        refs.pop(0)
        if own:
            send_ref, keep_ref, tok_ref, acc, recv_s, sem, recv_sem = refs
        else:
            g_ref, tok_ref, acc, sem = refs
        k = pl.program_id(0)
        n = no_ref[...] + nr_ref[...]
        c1 = jnp.minimum(1.0, cu_ref[layer] / jnp.sqrt(n[0, 0:1, 0:1]))
        c2 = jnp.minimum(1.0, cd_ref[layer] / jnp.sqrt(n[1, 0:1, 0:1]))
        y = s_ref[1]
        halves = (1 - y, y) if own else (0, 1)
        if own:
            recv_copy = pltpu.make_async_copy(recv_ref, recv_s, recv_sem)

        def copies(g, at):
            ds = block(halves[at], 512)
            if not own:
                part = (0, ds) if g == 0 else (1, slice(None), ds)
                return [pltpu.make_async_copy(acc.at[part], g_ref.at[part], sem.at[g, at, 0])]
            out = (send_ref, keep_ref)[at]
            if g == 0:
                return [pltpu.make_async_copy(acc.at[0, ds], out.at[0], sem.at[g, at, 0])]
            return [
                pltpu.make_async_copy(acc.at[1, pl.ds(b * 512, 512), ds], out.at[1, :, pl.ds(b * 512, 512)], sem.at[g, at, b])
                for b in range(2)
            ]

        @pl.when(k == 0)
        def _():
            tok_ref[...] = jnp.zeros((8, 128), F32)
            if own:
                recv_copy.start()

        def add(init, final):
            dhc = (dh_ref[...].astype(F32) * c1).astype(BF16)
            if final and own:
                recv_copy.wait()
            started = []
            for at in range(2):
                ds = block(halves[at], 512)
                for g in range(2):
                    if g == 0:
                        part = (0, ds)
                        new = lax.dot_general(x_ref[:, ds], dhc, TN, preferred_element_type=F32)
                    else:
                        part = (1, slice(None), ds)
                        new = lax.dot_general(h_ref[...], (dz_ref[:, ds].astype(F32) * c2).astype(BF16), TN, preferred_element_type=F32)
                    if not init:
                        new = acc[part] + new
                    if final and own:
                        new = new + recv_s[part]
                    acc[part] = new
                    if final:
                        if started:
                            for c in copies(*started[-1]):
                                c.start()
                        started.append((g, at))
            if final:
                for c in copies(*started[-1]):
                    c.start()
                for s in started:
                    for c in copies(*s):
                        c.wait()

        @pl.when(k == 0)
        def _():
            add(True, False)

        @pl.when((k > 0) & (k < steps - 1))
        def _():
            add(False, False)

        @pl.when(k == steps - 1)
        def _():
            add(False, True)

    norm_in = pl.BlockSpec((None, 2, 8, 128), lambda k, s: (k, 0, 0, 0))
    in_specs = [
        pl.BlockSpec((None, None, T, D), lambda k, s: (layer, s[0] * E + k, 0, 0)),
        pl.BlockSpec((None, T, Q), lambda k, s: (k, 0, half)),
        pl.BlockSpec((None, T, Q), lambda k, s: (k, 0, half)),
        pl.BlockSpec((None, T, D), lambda k, s: (k, 0, 0)),
        norm_in, norm_in, SMEM, SMEM,
    ]
    args = [x_all, dh, hid, dz, norms, norms_recv, clip_up, clip_down]
    piece = jax.ShapeDtypeStruct((2, 512, 1024), F32)
    scratch = [pltpu.VMEM((2, 1024, 1024), F32)]
    if own:
        in_specs.append(ANY)
        args.append(recv)
        out_shape, out_specs = [piece, piece, TOKEN], [ANY, ANY, TOKEN_SPEC]
        scratch += [pltpu.VMEM((2, 1024, 1024), F32), pltpu.SemaphoreType.DMA((2, 2, 2)), pltpu.SemaphoreType.DMA]
    else:
        out_shape, out_specs = [jax.ShapeDtypeStruct((2, 1024, 1024), F32), TOKEN], [ANY, TOKEN_SPEC]
        scratch += [pltpu.SemaphoreType.DMA((2, 2, 2))]
    return pl.pallas_call(
        body,
        out_shape=out_shape,
        grid_spec=pltpu.PrefetchScalarGridSpec(
            num_scalar_prefetch=1, grid=(steps,), in_specs=in_specs + [ANY], out_specs=out_specs, scratch_shapes=scratch,
        ),
        compiler_params=PARAMS,
    )(scal, *args, dep)


def weight_piece_call(layer, half, at, x_all, bufs, norms, norms_recv, clip_up, clip_down, scal, recv, dep):
    dz, dh, hid = bufs
    own = half == 0
    steps = E

    def body(*refs):
        refs = list(refs)
        _, x_ref, dh_ref, h_ref, dz_ref, no_ref, nr_ref, cu_ref, cd_ref = refs[:9]
        del refs[:9]
        if own:
            recv_ref = refs.pop(0)
        refs.pop(0)
        out_ref, tok_ref, acc1, acc2 = refs
        k = pl.program_id(0)
        n = no_ref[...] + nr_ref[...]
        c1 = jnp.minimum(1.0, cu_ref[layer] / jnp.sqrt(n[0, 0:1, 0:1]))
        c2 = jnp.minimum(1.0, cd_ref[layer] / jnp.sqrt(n[1, 0:1, 0:1]))

        def products():
            g1 = lax.dot_general(x_ref[...], (dh_ref[...].astype(F32) * c1).astype(BF16), TN, preferred_element_type=F32)
            g2 = lax.dot_general(h_ref[...], (dz_ref[...].astype(F32) * c2).astype(BF16), TN, preferred_element_type=F32)
            return g1, g2

        @pl.when(k == 0)
        def _():
            tok_ref[...] = jnp.zeros((8, 128), F32)
            acc1[...], acc2[...] = products()

        @pl.when((k > 0) & (k < steps - 1))
        def _():
            g1, g2 = products()
            acc1[...] += g1
            acc2[...] += g2

        @pl.when(k == steps - 1)
        def _():
            g1, g2 = products()
            g1 = acc1[...] + g1
            g2 = acc2[...] + g2
            if own:
                g1 = g1 + recv_ref[0]
            out_ref[0] = g1
            for b in range(2):
                cols = slice(b * 512, (b + 1) * 512)
                out_ref[1, :, cols] = g2[cols] + recv_ref[1, :, cols] if own else g2[cols]

    def d_half(s):
        return 1 - s[1] if at == 0 else s[1]

    norm_in = pl.BlockSpec((None, 2, 8, 128), lambda k, s: (k, 0, 0, 0))
    piece = pl.BlockSpec((2, 512, 1024), lambda k, s: (0, 0, 0))
    in_specs = [
        pl.BlockSpec((None, None, T, 512), lambda k, s: (layer, s[0] * E + k, 0, d_half(s))),
        pl.BlockSpec((None, T, Q), lambda k, s: (k, 0, half)),
        pl.BlockSpec((None, T, Q), lambda k, s: (k, 0, half)),
        pl.BlockSpec((None, T, 512), lambda k, s: (k, 0, d_half(s))),
        norm_in, norm_in, SMEM, SMEM,
    ]
    args = [x_all, dh, hid, dz, norms, norms_recv, clip_up, clip_down]
    if own:
        in_specs.append(piece)
        args.append(recv)
    return pl.pallas_call(
        body,
        out_shape=[jax.ShapeDtypeStruct((2, 512, 1024), F32), TOKEN],
        grid_spec=pltpu.PrefetchScalarGridSpec(
            num_scalar_prefetch=1, grid=(steps,), in_specs=in_specs + [ANY], out_specs=[piece, TOKEN_SPEC],
            scratch_shapes=[pltpu.VMEM((512, 1024), F32), pltpu.VMEM((1024, 512), F32)],
        ),
        compiler_params=PARAMS,
    )(scal, *args, dep)


def pack_call(layer, start, count, scal, u_all, dep, weights=()):
    nw = len(weights)

    def body(*refs):
        ins, outs = refs[1:2 + nw], refs[3 + nw:4 + 2 * nw]
        for a, b in zip(ins, outs):
            b[...] = a[...]
        refs[-1][...] = jnp.zeros((8, 128), F32)

    w_in = pl.BlockSpec((None, 512, 1024), lambda e, i, s: (layer, i, 0))
    w_out = pl.BlockSpec((None, 512, 1024), lambda e, i, s: (0, i, 0))
    return pl.pallas_call(
        body,
        out_shape=[jax.ShapeDtypeStruct((count, T, Q), BF16)] + [jax.ShapeDtypeStruct((1, 1024, 1024), BF16)] * nw + [TOKEN],
        grid_spec=pltpu.PrefetchScalarGridSpec(
            num_scalar_prefetch=1, grid=(count, 2),
            in_specs=[pl.BlockSpec((None, None, 512, Q), lambda e, i, s: (layer, (1 - s[0]) * E + start + e, i, 0))] + [w_in] * nw + [ANY],
            out_specs=[pl.BlockSpec((None, 512, Q), lambda e, i, s: (e, i, 0))] + [w_out] * nw + [TOKEN_SPEC],
        ),
        compiler_params=PARAMS,
    )(scal, u_all, *weights, dep)


def final_call(layer, num_layers, total, keep, y_recv, noise_up, noise_down, clip_up, clip_down, noise_mult, outs, dep):
    def body(*refs):
        k1, k2, y1, y2, n1, n2, cu, cd, sg = refs[:9]
        up, down, tok_ref = refs[-3:]
        up[...] = (k1[...] + y1[...] + (sg[0] * cu[layer]) * n1[...]) / total
        down[...] = (k2[...] + y2[...] + (sg[0] * cd[layer]) * n2[...]) / total
        tok_ref[...] = jnp.zeros((8, 128), F32)

    s1 = pl.BlockSpec((None, 512, 512), lambda j: (0, 0, j))
    s2 = pl.BlockSpec((None, 512, 512), lambda j: (1, 0, j))
    up_spec = pl.BlockSpec((None, 512, 512), lambda j: (layer, 0, j))
    down_spec = pl.BlockSpec((None, 512, 512), lambda j: (layer, j, 0))
    in_specs = [s1, s2, s1, s2, up_spec, down_spec, SMEM, SMEM, SMEM, ANY]
    args = [keep, keep, y_recv, y_recv, noise_up, noise_down, clip_up, clip_down, noise_mult, dep]
    aliases = {}
    if outs is not None:
        in_specs += [ANY, ANY]
        args += list(outs)
        aliases = {10: 0, 11: 1}
    up, down, tok = pl.pallas_call(
        body,
        out_shape=[jax.ShapeDtypeStruct((num_layers, 512, 1024), F32), jax.ShapeDtypeStruct((num_layers, 1024, 512), F32), TOKEN],
        grid=(2,),
        in_specs=in_specs,
        out_specs=[up_spec, down_spec, TOKEN_SPEC],
        input_output_aliases=aliases,
        compiler_params=PARAMS,
    )(*args)
    return (up, down), tok


def program_order(num_layers):
    top = num_layers - 1
    order = [("k", "pack", top, 0), ("p", "u", top, 0), ("p", "w", top, 0), ("p", "w", top, 1)]
    order += [("k", "pack", top, 1), ("p", "u", top, 1), ("p", "w", 0, 0), ("p", "w", 0, 1)]

    def give(layer):
        return [("k", "wgrad", layer, 1), ("p", "c", layer, 0)]

    def own(layer):
        return [("k", "wgrad", layer, 0), ("p", "y", layer, 0)]

    for layer in range(top, 0, -1):
        if layer == top:
            order += [("k", "chaina", layer, 0), ("p", "xa", layer, 0), ("k", "chainb", layer, 0), ("p", "xb", layer, 0), ("k", "norm", layer, 0)]
        else:
            order += [("k", "chain", layer, 0), ("p", "x", layer, 0)]
        order.append(("k", "chain", layer, 1))
        if layer > 1:
            order.append(("p", "x", layer, 1))
        order.append(("p", "u", layer - 1, E))
        if layer == 1:
            order.append(("k", "chain", 1, 2))
        if layer < top:
            order += give(layer + 1)
        if layer > 1:
            order += [("k", "pair", layer, 2), ("p", "n", layer, 0)]
            order += [("p", "x", layer, 2)] if layer > 2 else [("p", "x", 2, 2), ("p", "x", 2, 3)]
        else:
            order += [("k", "chain", 1, 3), ("p", "n", 1, 0), ("p", "x", 1, 1), ("p", "x", 1, 2), ("p", "x", 1, 3)]
        if 1 < layer < top - 1:
            order.append(("k", "final", layer + 2, 0))
        if layer < top:
            order += own(layer + 1)
    order += give(1) + [("k", "chain", 0, 0)] + own(1) + [("k", "chain", 0, 1), ("k", "chain", 0, 2), ("k", "final", 3, 0), ("k", "chain", 0, 3), ("p", "n", 0, 0)]
    order += [("k", "piece1", 0, 0), ("p", "c", 0, 0), ("k", "final", 2, 0), ("k", "piece0", 0, 0), ("p", "y", 0, 0)]
    order += [("k", "piece1", 0, 1), ("p", "c", 0, 1), ("k", "final", 1, 0), ("k", "piece0", 0, 1), ("k", "final", 0, 0)]
    return order


def solution(mesh):
    in_specs = (P(None, "dp", None, None), P(None, "dp", None, "tp"), P(None, None, "tp"), P(None, "tp", None), P("dp", None, None), P(None, "dp", "tp"), P(None, "tp", "dp"), P(), P(), P())
    out_specs = (P(None, "dp", "tp"), P(None, "tp", "dp"))
    swap_core = [(0, 1), (1, 0), (2, 3), (3, 2)]
    swap_x = [(0, 2), (2, 0), (1, 3), (3, 1)]
    swap_dp = [(0, 1), (1, 0)]
    num_layers = 6

    def local_step(x_stored, u_stored, w_up, w_down, d_out, noise_up, noise_down, clip_up, clip_down, noise_mult):
        total = float(d_out.shape[0] * mesh.shape["dp"])
        top = num_layers - 1
        scal = jnp.stack([lax.axis_index("tp") % 2, lax.axis_index("dp")]).astype(jnp.int32)
        tok = jnp.zeros((8, 128), F32)
        bufs, norms, part, part_recv, packed, u_recv, w_pack, w_recv = {}, {}, {}, {}, {}, {}, {}, {}
        pieces = {}
        norms_recv, give, recv, y_send, keep, y_recv = {}, {}, {}, {}, {}, {}
        outs = None
        for step in program_order(num_layers):
            kind, what, layer, k = step
            first, last = layer == top, layer == 0
            if kind == "p":
                if what == "u":
                    u_recv[layer, k] = lax.ppermute(packed[layer, k], "tp", swap_core)
                elif what == "w":
                    w_recv[layer, k] = lax.ppermute(w_pack[k] if first else (w_down, w_up)[k], "tp", swap_core)
                elif what == "n":
                    norms_recv[layer] = lax.ppermute(norms[layer], "tp", swap_x)
                elif what in ("x", "xa", "xb"):
                    part_recv[layer, what, k] = lax.ppermute(part[layer, what, k], "tp", swap_x)
                elif what == "c":
                    if last:
                        pieces[2, k] = lax.ppermute(pieces[1, k], "tp", swap_core)
                    else:
                        recv[layer] = lax.ppermute(give[layer], "tp", swap_core)
                else:
                    y_recv[layer] = lax.ppermute(y_send[layer], "dp", swap_dp)
            elif what == "pack":
                if first and k == 0:
                    packed[layer, k], w_pack[0], w_pack[1], tok = pack_call(layer, 0, 1, scal, u_stored, tok, (w_down, w_up))
                else:
                    packed[layer, k], tok = pack_call(layer, 1, E - 1, scal, u_stored, tok)
            elif what in ("chain", "chaina", "chainb", "pair"):
                w_at = top if first else 0
                exs = (2, 3) if what == "pair" else (k,)
                blocks = {"chaina": (0,), "chainb": (1,)}.get(what, (0, 1))
                apart = what == "pair" and layer == 2
                sources = {}
                for e in exs:
                    for i in range(NB):
                        rows = pl.ds(i * TB, TB)
                        if first:
                            continue
                        if (layer + 1, "xa", e) in part:
                            at, index = (layer + 1, ("xa", "xb")[i], e), pl.ds(0, TB)
                        elif (layer + 1, "x", e) in part and part[layer + 1, "x", e].ndim == 2:
                            at, index = (layer + 1, "x", e), rows
                        else:
                            at, index = (layer + 1, "x", 2), (e - 2, rows)
                        sources[e, i] = (f"{at[1]}{at[2]}", part[at], part_recv[at], index)
                bufs[layer], norms[layer], sent, packed[layer - 1, E], tok = chain_call(
                    layer, exs, blocks, first, last, len(blocks) == NB, layer > 0 and k < 2 and what != "chainb", apart, scal,
                    d_out if first else bufs[layer + 1][0], sources, u_stored, u_recv[layer, min(k, 1) if first else E], x_stored,
                    w_down, w_recv[w_at, 0], w_up, w_recv[w_at, 1], bufs.get(layer), norms.get(layer), packed.get((layer - 1, E)), tok,
                )
                for j, a in enumerate(sent):
                    part[layer, {"chaina": "xa", "chainb": "xb"}.get(what, "x"), k + j] = a
            elif what == "norm":
                norms[layer], tok = norm_call(layer, k, scal, x_stored, bufs[layer], tok)
            elif what == "wgrad":
                got = weight_call(
                    layer, k, x_stored, bufs[layer], norms[layer], norms_recv[layer], clip_up, clip_down, scal, recv.get(layer), tok
                )
                tok = got[-1]
                if k == 1:
                    give[layer] = got[0]
                else:
                    y_send[layer], keep[layer] = got[:2]
            elif what in ("piece1", "piece0"):
                half = int(what[-1])
                pieces[half, k], tok = weight_piece_call(
                    layer, half, k, x_stored, bufs[layer], norms[layer], norms_recv[layer], clip_up, clip_down, scal, pieces.get((2, k)), tok
                )
                if half == 0:
                    (y_send, keep)[k][layer] = pieces[0, k]
            else:
                outs, tok = final_call(
                    layer, num_layers, total, keep[layer], y_recv[layer], noise_up, noise_down, clip_up, clip_down, noise_mult, outs, tok
                )
        return outs

    return jax.shard_map(local_step, mesh=mesh, in_specs=in_specs, out_specs=out_specs, check_vma=False)
```
